256 devices in a mesh: slab: 32 (over z, y), energy: 8 (over x, core).
Axes of the slice: x: 4, y: 4, z: 8, core: 2. Of those that a mesh axis runs over, the one named last changes fastest.
Arguments:
- green: bfloat16 [8, 32, 3, 2, 384, 384], P('energy', 'slab'), may hold values from -0.3125 to 0.3125
- sigma: bfloat16 [8, 32, 3, 2, 384, 384], P('energy', 'slab'), may hold values from -4 to 4
- phonon: bfloat16 [8, 32, 2, 384, 384], P('energy', 'slab'), may hold values from -4 to 4
- pair_off: int32 [32, 3], replicated, may hold values from -2 to 2, as said below
- pair_count: int32 [32], replicated, may hold values from 1 to 3, as said below
- pair_range: int32 [32, 3], replicated, may hold values from 96 to 384, as said below
Outputs:
- lesser: float32 [8, 32, 2, 384, 384], P('energy', 'slab')
The draws below stay inside these ranges and needn't reach their ends.
Inputs may be any that keep to these rules, and one draw needn't show every extreme that they name: The partner slab k + pair_off[k, q] lies inside the grid. `pair_count`: some slab has 3 live slots. `pair_range`: a multiple of 96; some pair couples all 384 orbitals.
All inputs are finite; a program needn't handle non-finite values.
Results may differ from the reference program's by a relative error of at most 0.0035.
Values may be sent and summed in bfloat16 or wider, within the bound.
No kernel may reach another device: no remote copies, remote signals or barrier semaphores. Data moves between devices by JAX's collectives and lax.ppermute only.
A program may use at most 64 MiB of HBM per device.

```python
import jax
import jax.numpy as jnp
from jax import lax

ORB = 384
MAXP = 3
NSLAB = 32
EN = 8


def draw_pair_off(key, part):
    shifts = jax.random.randint(key, (NSLAB, MAXP), -2, 3).astype(jnp.int32)
    slab_ids = jnp.arange(NSLAB, dtype=jnp.int32)[:, None]
    partner = slab_ids + shifts
    outside = (partner < 0) | (partner >= NSLAB)
    return jnp.where(outside, -shifts, shifts).astype(jnp.int32)


def draw_pair_count(key, part):
    counts = jax.random.randint(jax.random.fold_in(key, 11), (NSLAB,), 1, MAXP + 1).astype(jnp.int32)
    fullest = jax.random.randint(jax.random.fold_in(key, 12), (), 0, NSLAB)
    return counts.at[fullest].set(MAXP).astype(jnp.int32)


def draw_pair_range(key, part):
    quarters = jax.random.randint(jax.random.fold_in(key, 21), (NSLAB, MAXP), 1, 5).astype(jnp.int32)
    widest = jax.random.randint(jax.random.fold_in(key, 22), (), 0, NSLAB)
    quarters = quarters.at[widest, 0].set(4)
    return (quarters * (ORB // 4)).astype(jnp.int32)


def block_levels(own_key, dims, split, low, largest):
    loudness = 1.0
    for dim, parts in split:
        heights = jax.random.uniform(jax.random.fold_in(jax.random.fold_in(own_key, 6), dim), (parts,), jnp.float32, low / len(split), largest / len(split))
        loudness = loudness * jnp.repeat(jnp.exp(heights), dims[dim] // parts).reshape((-1,) + (1,) * (len(dims) - 1 - dim))
    return loudness


def bell_draw(own_key, shape, spread, most, pieces=(), kind=jnp.bfloat16):
    entries = jax.random.normal(own_key, shape, jnp.float32) * spread
    if len(pieces) > 0:
        entries = block_levels(own_key, shape, pieces, -0.22, 0.18) * entries
    return jnp.clip(entries, min=-most, max=most).astype(kind)


def setup_inputs(seed: int = 0) -> dict:
    keys = jax.random.split(jax.random.key(seed), 7)
    green = bell_draw(keys[0], (EN, NSLAB, 3, 2, ORB, ORB), ORB ** -0.5, 0.3125, ((0, 8), (1, 32)))
    sigma = bell_draw(keys[1], (EN, NSLAB, MAXP, 2, ORB, ORB), 0.3, 4.0, ((0, 8), (1, 32)))
    phonon = bell_draw(keys[2], (EN, NSLAB, 2, ORB, ORB), 0.3, 4.0, ((0, 8), (1, 32)))
    pair_off = draw_pair_off(jax.random.fold_in(keys[6], 71), 0)
    pair_count = draw_pair_count(jax.random.fold_in(keys[6], 71), 0)
    pair_range = draw_pair_range(jax.random.fold_in(keys[6], 71), 0)
    return {"green": green, "sigma": sigma, "phonon": phonon, "pair_off": pair_off, "pair_count": pair_count, "pair_range": pair_range}


def conj_sum(source, chosen):
    real = jnp.einsum('qmn,qpn->mp', source[:, 0], chosen[:, 0]) + jnp.einsum('qmn,qpn->mp', source[:, 1], chosen[:, 1])
    imag = jnp.einsum('qmn,qpn->mp', source[:, 1], chosen[:, 0]) - jnp.einsum('qmn,qpn->mp', source[:, 0], chosen[:, 1])
    return real, imag


def complex_times(left, real, imag):
    first = jnp.dot(left[0], real, preferred_element_type=jnp.float32) - jnp.dot(left[1], imag, preferred_element_type=jnp.float32)
    second = jnp.dot(left[0], imag, preferred_element_type=jnp.float32) + jnp.dot(left[1], real, preferred_element_type=jnp.float32)
    return jnp.stack([first, second])


def reference(green, sigma, phonon, pair_off, pair_count, pair_range):
    slab_total = green.shape[1]
    width = green.shape[-1]
    slots = pair_off.shape[1]
    positions = jnp.arange(width, dtype=jnp.int32)
    inside = positions[None, None, :] < pair_range[:, :, None]
    square = inside[:, :, :, None] & inside[:, :, None, :]
    masked = jnp.where(square[None, :, :, None], sigma, jnp.zeros((), jnp.bfloat16))
    padded = jnp.pad(phonon.astype(jnp.float32), ((1, 1), (0, 0), (0, 0), (0, 0), (0, 0)))
    phonon_mix = (0.5 * (padded[:-2] + padded[2:])).astype(jnp.bfloat16)
    sources = jnp.concatenate([masked, phonon_mix[:, :, None]], axis=2)
    slot_ids = jnp.arange(slots, dtype=jnp.int32)

    def one_row(flat):
        energy = flat // slab_total
        slab = flat % slab_total
        green_row = green[energy, slab]
        running = jnp.zeros((2, width, width), jnp.float32)
        for delta in (-1, 0, 1):
            other = (slab + delta).astype(jnp.int32)
            clipped = jnp.clip(other, 0, slab_total - 1).astype(jnp.int32)
            valid = (other >= 0) & (other < slab_total)
            source = sources[energy, clipped].astype(jnp.float32)
            offsets = pair_off[clipped]
            count = pair_count[clipped]
            place = (clipped + offsets - slab + 1).astype(jnp.int32)
            usable = (place >= 0) & (place <= 2) & (slot_ids < count)
            pick = jnp.concatenate([jnp.clip(place, 0, 2).astype(jnp.int32), jnp.array([delta + 1], jnp.int32)])
            keep = jnp.concatenate([usable, jnp.array([True])]).astype(jnp.float32)
            chosen = green_row[pick].astype(jnp.float32) * keep[:, None, None, None]
            real, imag = conj_sum(source, chosen)
            term = complex_times(green_row[delta + 1], real.astype(jnp.bfloat16), imag.astype(jnp.bfloat16))
            running = running + jnp.where(valid, term, jnp.zeros_like(term))
        return running

    flat_ids = jnp.arange(green.shape[0] * slab_total, dtype=jnp.int32)
    result = lax.map(one_row, flat_ids)
    return result.reshape(green.shape[0], slab_total, 2, width, width)
```

```python
import jax
import jax.numpy as jnp
from jax import lax
from jax.experimental import pallas as pl
from jax.experimental.pallas import tpu as pltpu
from jax.sharding import PartitionSpec as P

F32 = jnp.float32
BF16 = jnp.bfloat16
VMEM_LIMIT = 24 * 1024 * 1024


def cost(flops, moved):
    return pl.CostEstimate(flops=int(flops), bytes_accessed=int(moved), transcendentals=0)


def dot(left, right):
    return jnp.dot(left, right, preferred_element_type=F32)


def pair_limit(slab, offset, q, off, cnt, rng):
    live = (off[slab, q] == offset) & (q < cnt[slab])
    return jnp.where(live, rng[slab, q], 0)


def merged(slab, offset, sigma, part, rows, cols, off, cnt, rng):
    total = jnp.zeros(rows.shape, F32)
    for q in range(sigma.shape[2]):
        limit = pair_limit(slab, offset, q, off, cnt, rng)
        inside = (rows < limit) & (cols < limit)
        total = total + jnp.where(inside, sigma[0, 0, q, part].astype(F32), 0.0)
    return total


def index_grid(first, height, width):
    rows = lax.broadcasted_iota(jnp.int32, (height, width), 0) + first
    cols = lax.broadcasted_iota(jnp.int32, (height, width), 1)
    return rows, cols


def side_kernel(off, cnt, rng, sigma, low, high):
    slab = lax.axis_index("slab")
    height, width = sigma.shape[-2:]
    rows, cols = index_grid(pl.program_id(0) * height, height, width)
    for out, offsets in ((low, (-2, -1)), (high, (1, 2))):
        for slot, offset in enumerate(offsets):
            for part in range(2):
                block = merged(slab, offset, sigma, part, rows, cols, off, cnt, rng)
                at = (2 * slot + part) * width
                out[:, at : at + width] = block.astype(BF16)


def centre_kernel(off, cnt, rng, sigma, below, above, out):
    slab = lax.axis_index("slab")
    height, width = sigma.shape[-2:]
    rows, cols = index_grid(pl.program_id(0) * height, height, width)
    for part in range(2):
        block = merged(slab, 0, sigma, part, rows, cols, off, cnt, rng)
        mixed = 0.5 * (below[0, 0, part].astype(F32) + above[0, 0, part].astype(F32))
        block = block + mixed.astype(BF16).astype(F32)
        out[:, part * width : (part + 1) * width] = block.astype(BF16)


def green_kernel(green, right, left):
    width = green.shape[-1]
    for o in range(3):
        real, imag = green[0, 0, o, 0], green[0, 0, o, 1]
        real_t, imag_t = real.T, imag.T
        at = 2 * o * width
        right[at : at + width, :width] = real_t
        right[at : at + width, width:] = -imag_t
        right[at + width : at + 2 * width, :width] = imag_t
        right[at + width : at + 2 * width, width:] = real_t
        to = 2 * ((o + 1) % 3) * width
        left[:, to : to + width] = real
        left[:, to + width : to + 2 * width] = imag


def spread(x, out, first):
    width = x.shape[1] // 2
    rounded = x.astype(BF16)
    real, imag = rounded[:, :width], rounded[:, width:]
    out[first : first + width, :width] = real
    out[first : first + width, width:] = imag
    out[first + width : first + 2 * width, :width] = -imag
    out[first + width : first + 2 * width, width:] = real


def local_kernel(low, centre, high, right, left, out, held):
    wide = centre.shape[1]
    x = dot(low[:, wide:], right[:wide])
    x = x + dot(centre[...], right[wide : 2 * wide])
    x = x + dot(high[:, :wide], right[2 * wide :])
    spread(x, held, 0)
    out[...] = dot(left[:, 2 * wide :], held[...])


def arrive_kernel(from_above, from_below, right, out_above, out_below):
    wide = from_above.shape[1]
    out_above[...] = dot(from_above[...], right[:wide])
    out_below[...] = dot(from_below[...], right[wide // 2 :])


def finish_kernel(centre_above, centre_below, x_above, x_below, right, left, partial, out, held):
    wide = centre_above.shape[1]
    width = wide // 2
    above = x_above[...] + dot(centre_above[...], right[2 * wide :])
    below = x_below[...] + dot(centre_below[...], right[:wide])
    spread(above, held, 0)
    spread(below, held, wide)
    total = partial[...] + dot(left[:, : 2 * wide], held[...])
    out[0, 0, 0] = total[:, :width]
    out[0, 0, 1] = total[:, width:]


def smem():
    return pl.BlockSpec(memory_space=pltpu.SMEM)


def params():
    return pltpu.CompilerParams(vmem_limit_bytes=VMEM_LIMIT)


def body(green, sigma, phonon, pair_off, pair_count, pair_range):
    width = green.shape[-1]
    wide = 2 * width
    slots = sigma.shape[2]
    slabs = lax.axis_size("slab")
    points = lax.axis_size("energy")
    up = [(i, i + 1) for i in range(slabs - 1)]
    down = [(i + 1, i) for i in range(slabs - 1)]
    energy_up = [(i, i + 1) for i in range(points - 1)]
    energy_down = [(i + 1, i) for i in range(points - 1)]
    tables = (pair_off, pair_count, pair_range)

    ph_below = lax.ppermute(phonon, "energy", energy_up)
    ph_above = lax.ppermute(phonon, "energy", energy_down)

    height = 128
    steps = width // height
    sigma_spec = pl.BlockSpec((1, 1, slots, 2, height, width), lambda s: (0, 0, 0, 0, s, 0))
    phonon_spec = pl.BlockSpec((1, 1, 2, height, width), lambda s: (0, 0, 0, s, 0))
    side_spec = pl.BlockSpec((height, 2 * wide), lambda s: (s, 0))
    block_bytes = 2 * width * wide
    low, high = pl.pallas_call(
        side_kernel,
        grid=(steps,),
        in_specs=[smem(), smem(), smem(), sigma_spec],
        out_specs=[side_spec, side_spec],
        out_shape=[jax.ShapeDtypeStruct((width, 2 * wide), BF16)] * 2,
        compiler_params=params(),
        cost_estimate=cost(3e9, 7 * block_bytes),
        name="side",
    )(*tables, sigma)
    low_above = lax.ppermute(low, "slab", down)
    high_below = lax.ppermute(high, "slab", up)

    centre = pl.pallas_call(
        centre_kernel,
        grid=(steps,),
        in_specs=[smem(), smem(), smem(), sigma_spec, phonon_spec, phonon_spec],
        out_specs=pl.BlockSpec((height, wide), lambda s: (s, 0)),
        out_shape=jax.ShapeDtypeStruct((width, wide), BF16),
        compiler_params=params(),
        cost_estimate=cost(3e9, 6 * block_bytes),
        name="centre",
    )(*tables, sigma, ph_below, ph_above)
    centre_above = lax.ppermute(centre, "slab", down)
    centre_below = lax.ppermute(centre, "slab", up)

    right, left = pl.pallas_call(
        green_kernel,
        out_shape=[
            jax.ShapeDtypeStruct((3 * wide, wide), BF16),
            jax.ShapeDtypeStruct((width, 3 * wide), BF16),
        ],
        compiler_params=params(),
        cost_estimate=cost(4e9, 12 * block_bytes),
        name="green",
    )(green)

    square = jax.ShapeDtypeStruct((width, wide), F32)
    partial = pl.pallas_call(
        local_kernel,
        out_shape=square,
        scratch_shapes=[pltpu.VMEM((wide, wide), BF16)],
        compiler_params=params(),
        cost_estimate=cost(2 * width * wide * 4 * wide, 16 * block_bytes),
        name="local",
    )(low, centre, high, right, left)

    x_above, x_below = pl.pallas_call(
        arrive_kernel,
        out_shape=[square, square],
        compiler_params=params(),
        cost_estimate=cost(2 * width * wide * 4 * wide, 16 * block_bytes),
        name="arrive",
    )(low_above, high_below, right)

    return pl.pallas_call(
        finish_kernel,
        out_shape=jax.ShapeDtypeStruct((1, 1, 2, width, width), F32),
        scratch_shapes=[pltpu.VMEM((2 * wide, wide), BF16)],
        compiler_params=params(),
        cost_estimate=cost(2 * width * wide * 4 * wide, 16 * block_bytes),
        name="finish",
    )(centre_above, centre_below, x_above, x_below, right, left, partial)


def solution(mesh):
    in_specs = (
        P("energy", "slab", None, None, None, None),
        P("energy", "slab", None, None, None, None),
        P("energy", "slab", None, None, None),
        P(),
        P(),
        P(),
    )
    out_specs = P("energy", "slab", None, None, None)
    return jax.shard_map(body, mesh=mesh, in_specs=in_specs, out_specs=out_specs, check_vma=False)
```

```python
import jax
import jax.numpy as jnp
from jax import lax
from jax.experimental import pallas as pl
from jax.experimental.pallas import tpu as pltpu
from jax.sharding import PartitionSpec as P


F32 = jnp.float32
BF16 = jnp.bfloat16
VMEM_LIMIT = 24 * 1024 * 1024
CHUNKS = 3


def cost(flops, moved):
    return pl.CostEstimate(flops=int(flops), bytes_accessed=int(moved), transcendentals=0)


def dot(left, right):
    return jnp.dot(left, right, preferred_element_type=F32)


def toward():
    return 1 - 2 * lax.rem(lax.axis_index("slab"), 2)


def matches(slab, offset, off, cnt, rng):
    found = []
    for q in range(off.shape[0]):
        live = (off[q, slab] == offset) & (q < cnt[slab])
        found.append((live.astype(jnp.int32), jnp.where(live, rng[q, slab], 0)))
    return found


def masked(block, rows, cols, limit):
    return jnp.where((rows < limit) & (cols < limit), block.astype(F32), 0.0)


def index_grid(first, height, width):
    rows = lax.broadcasted_iota(jnp.int32, (height, width), 0) + first
    cols = lax.broadcasted_iota(jnp.int32, (height, width), 1)
    return rows, cols


def side_kernel(off_in, cnt_in, rng_in, sigma, first, second, off, cnt, rng, held, sems, table_sems):
    slab = lax.axis_index("slab")
    s = toward()
    chunks, slots, _, height, width = held.shape
    tables = [
        pltpu.make_async_copy(src, dst, table_sems.at[n])
        for n, (src, dst) in enumerate(((off_in, off), (cnt_in, cnt), (rng_in, rng)))
    ]
    copies = [
        pltpu.make_async_copy(
            sigma.at[0, 0, :, :, pl.ds(c * height, height), :], held.at[c], sems.at[c]
        )
        for c in range(chunks)
    ]
    for copy in tables + copies:
        copy.start()
    for copy in tables:
        copy.wait()
    wanted = (
        (first, 0, s),
        (first, 1, 2 * s),
        (second, 0, -2 * s),
        (second, 1, -s),
    )
    for c in range(chunks):
        copies[c].wait()
        rows, cols = index_grid(c * height, height, width)
        top = pl.ds(c * height, height)
        for out, slot, offset in wanted:
            found = matches(slab, offset, off, cnt, rng)
            number = sum(live for live, _ in found)
            which = sum(q * live for q, (live, _) in enumerate(found))
            limit = sum(reach for _, reach in found)
            at = [pl.ds((2 * slot + part) * width, width) for part in range(2)]

            @pl.when(number == 0)
            def _():
                for part in range(2):
                    out[top, at[part]] = jnp.zeros((height, width), BF16)

            @pl.when(number == 1)
            def _():
                for part in range(2):
                    out[top, at[part]] = masked(held[c, which, part], rows, cols, limit).astype(BF16)

            @pl.when(number > 1)
            def _():
                for part in range(2):
                    total = jnp.zeros((height, width), F32)
                    for q in range(slots):
                        total = total + masked(held[c, q, part], rows, cols, found[q][1])
                    out[top, at[part]] = total.astype(BF16)


def centre_kernel(off, cnt, rng, sigma, one, two, out):
    slab = lax.axis_index("slab")
    height, width = sigma.shape[-2:]
    rows, cols = index_grid(pl.program_id(0) * height, height, width)
    found = matches(slab, 0, off, cnt, rng)
    for part in range(2):
        mixed = 0.5 * (one[0, 0, part].astype(F32) + two[0, 0, part].astype(F32))
        total = mixed.astype(BF16).astype(F32)
        for q in range(sigma.shape[2]):
            total = total + masked(sigma[0, 0, q, part], rows, cols, found[q][1])
        out[:, part * width : (part + 1) * width] = total.astype(BF16)


def green_kernel(green, right, left):
    width = green.shape[-1]
    s = toward()
    for slot, (o, to) in enumerate(((1 + s, 0), (1, 2), (1 - s, 1))):
        real, imag = green[0, 0, o, 0], green[0, 0, o, 1]
        real_t, imag_t = real.T, imag.T
        at = 2 * slot * width
        right[at : at + width, :width] = real_t
        right[at : at + width, width:] = -imag_t
        right[at + width : at + 2 * width, :width] = imag_t
        right[at + width : at + 2 * width, width:] = real_t
        left[:, 2 * to * width : (2 * to + 1) * width] = real
        left[:, (2 * to + 1) * width : (2 * to + 2) * width] = imag


def spread(x, out, first):
    width = x.shape[1] // 2
    rounded = x.astype(BF16)
    real, imag = rounded[:, :width], rounded[:, width:]
    out[first : first + width, :width] = real
    out[first : first + width, width:] = imag
    out[first + width : first + 2 * width, :width] = -imag
    out[first + width : first + 2 * width, width:] = real


def local_kernel(first, centre, second, right, left, out, held):
    wide = centre.shape[1]
    x = dot(first[:, :wide], right[:wide])
    x = x + dot(centre[...], right[wide : 2 * wide])
    x = x + dot(second[:, wide:], right[2 * wide :])
    spread(x, held, 0)
    out[...] = dot(left[:, 2 * wide :], held[...])


def arrive_kernel(from_first, from_second, right, out_first, out_second):
    wide = out_first.shape[1]
    out_first[...] = dot(from_first[...], right[wide:])
    out_second[...] = dot(from_second[...], right[: 2 * wide])


def finish_kernel(c_first, c_second, x_first, x_second, right, left, partial, out, held, stage, sems):
    wide = c_first.shape[1]
    width = wide // 2
    spread(x_first[...] + dot(c_first[...], right[:wide]), held, 0)
    spread(x_second[...] + dot(c_second[...], right[2 * wide :]), held, wide)
    height = width // CHUNKS
    copies = []
    for c in range(CHUNKS):
        top = pl.ds(c * height, height)
        total = partial[top, :] + dot(left[top, : 2 * wide], held[...])
        stage[0, top, :] = total[:, :width]
        stage[1, top, :] = total[:, width:]
        copies.append(
            pltpu.make_async_copy(stage.at[:, top, :], out.at[0, 0, :, top, :], sems.at[c])
        )
        copies[-1].start()
    for copy in copies:
        copy.wait()


def smem():
    return pl.BlockSpec(memory_space=pltpu.SMEM)


def hbm():
    return pl.BlockSpec(memory_space=pltpu.HBM)


def params():
    return pltpu.CompilerParams(vmem_limit_bytes=VMEM_LIMIT)


def swaps(first, count):
    pairs = []
    for i in range(first, count - 1, 2):
        pairs += [(i, i + 1), (i + 1, i)]
    return pairs


def swap(value, axis, first):
    return lax.ppermute(value, axis, swaps(first, lax.axis_size(axis)))


def in_hbm(value):
    return pltpu.with_memory_space_constraint(value, pltpu.HBM)


def program(green, sigma, phonon, pair_off, pair_count, pair_range):
    width = green.shape[-1]
    wide = 2 * width
    slots = sigma.shape[2]
    tables = (pair_off.T, pair_count, pair_range.T)
    block_bytes = 2 * width * wide
    height = width // CHUNKS

    first, second = pl.pallas_call(
        side_kernel,
        in_specs=[hbm()] * 4,
        out_shape=[jax.ShapeDtypeStruct((width, 2 * wide), BF16)] * 2,
        scratch_shapes=[
            pltpu.SMEM(tables[0].shape, jnp.int32),
            pltpu.SMEM(tables[1].shape, jnp.int32),
            pltpu.SMEM(tables[2].shape, jnp.int32),
            pltpu.VMEM((CHUNKS, slots, 2, height, width), BF16),
            pltpu.SemaphoreType.DMA((CHUNKS,)),
            pltpu.SemaphoreType.DMA((3,)),
        ],
        compiler_params=params(),
        cost_estimate=cost(3e9, 7 * block_bytes),
        name="side",
    )(*[in_hbm(value) for value in (*tables, sigma)])
    from_first = swap(first, "slab", 0)
    from_second = swap(second, "slab", 1)

    one = swap(phonon, "energy", 0)
    two = swap(phonon, "energy", 1)

    sigma_spec = pl.BlockSpec((1, 1, slots, 2, height, width), lambda c: (0, 0, 0, 0, c, 0))
    phonon_spec = pl.BlockSpec((1, 1, 2, height, width), lambda c: (0, 0, 0, c, 0))
    centre = pl.pallas_call(
        centre_kernel,
        grid=(CHUNKS,),
        in_specs=[smem(), smem(), smem(), sigma_spec, phonon_spec, phonon_spec],
        out_specs=pl.BlockSpec((height, wide), lambda c: (c, 0)),
        out_shape=jax.ShapeDtypeStruct((width, wide), BF16),
        compiler_params=params(),
        cost_estimate=cost(3e9, 6 * block_bytes),
        name="centre",
    )(*[in_hbm(value) for value in (*tables, sigma)], one, two)
    c_first = swap(centre, "slab", 0)
    c_second = swap(centre, "slab", 1)

    right, left = pl.pallas_call(
        green_kernel,
        out_shape=[
            jax.ShapeDtypeStruct((3 * wide, wide), BF16),
            jax.ShapeDtypeStruct((width, 3 * wide), BF16),
        ],
        compiler_params=params(),
        cost_estimate=cost(4e9, 12 * block_bytes),
        name="green",
    )(green)

    square = jax.ShapeDtypeStruct((width, wide), F32)
    partial = pl.pallas_call(
        local_kernel,
        out_shape=square,
        scratch_shapes=[pltpu.VMEM((wide, wide), BF16)],
        compiler_params=params(),
        cost_estimate=cost(2 * width * wide * 4 * wide, 16 * block_bytes),
        name="local",
    )(first, centre, second, right, left)

    x_first, x_second = pl.pallas_call(
        arrive_kernel,
        out_shape=[square, square],
        compiler_params=params(),
        cost_estimate=cost(2 * width * wide * 4 * wide, 16 * block_bytes),
        name="arrive",
    )(from_first, from_second, right)

    return pl.pallas_call(
        finish_kernel,
        out_specs=hbm(),
        out_shape=jax.ShapeDtypeStruct((1, 1, 2, width, width), F32),
        scratch_shapes=[
            pltpu.VMEM((2 * wide, wide), BF16),
            pltpu.VMEM((2, width, width), F32),
            pltpu.SemaphoreType.DMA((CHUNKS,)),
        ],
        compiler_params=params(),
        cost_estimate=cost(2 * width * wide * 4 * wide, 16 * block_bytes),
        name="finish",
    )(c_first, c_second, x_first, x_second, right, left, partial)


def solution(mesh):
    in_specs = (
        P("energy", "slab", None, None, None, None),
        P("energy", "slab", None, None, None, None),
        P("energy", "slab", None, None, None),
        P(),
        P(),
        P(),
    )
    out_specs = P("energy", "slab", None, None, None)
    return jax.shard_map(program, mesh=mesh, in_specs=in_specs, out_specs=out_specs, check_vma=False)
```

```python
import jax
import jax.numpy as jnp
from jax import lax
from jax.experimental import pallas as pl
from jax.experimental.pallas import tpu as pltpu
from jax.sharding import PartitionSpec as P


F32 = jnp.float32
BF16 = jnp.bfloat16
VMEM_LIMIT = 24 * 1024 * 1024
CHUNKS = 3
SPLIT = 256


def cost(flops, moved):
    return pl.CostEstimate(flops=int(flops), bytes_accessed=int(moved), transcendentals=0)


def dot(left, right):
    return jnp.dot(left, right, preferred_element_type=F32)


def toward():
    return 1 - 2 * lax.rem(lax.axis_index("slab"), 2)


def matches(slab, offset, off, cnt, rng):
    found = []
    for q in range(off.shape[0]):
        live = (off[q, slab] == offset) & (q < cnt[slab])
        found.append((live.astype(jnp.int32), jnp.where(live, rng[q, slab], 0)))
    return found


def masked(block, rows, cols, limit):
    return jnp.where((rows < limit) & (cols < limit), block.astype(F32), 0.0)


def index_grid(first, height, width):
    rows = lax.broadcasted_iota(jnp.int32, (height, width), 0) + first
    cols = lax.broadcasted_iota(jnp.int32, (height, width), 1)
    return rows, cols


def side_kernel(off_in, cnt_in, rng_in, sigma, first, second, off, cnt, rng, held, sems, table_sems):
    slab = lax.axis_index("slab")
    s = toward()
    chunks, slots, _, height, width = held.shape
    tables = [
        pltpu.make_async_copy(src, dst, table_sems.at[n])
        for n, (src, dst) in enumerate(((off_in, off), (cnt_in, cnt), (rng_in, rng)))
    ]
    copies = [
        pltpu.make_async_copy(
            sigma.at[0, 0, :, :, pl.ds(c * height, height), :], held.at[c], sems.at[c]
        )
        for c in range(chunks)
    ]
    for copy in tables + copies:
        copy.start()
    for copy in tables:
        copy.wait()
    wanted = (
        (first, 0, s),
        (first, 1, 2 * s),
        (second, 0, -2 * s),
        (second, 1, -s),
    )
    for c in range(chunks):
        copies[c].wait()
        rows, cols = index_grid(c * height, height, width)
        top = pl.ds(c * height, height)
        for out, slot, offset in wanted:
            found = matches(slab, offset, off, cnt, rng)
            number = sum(live for live, _ in found)
            which = sum(q * live for q, (live, _) in enumerate(found))
            limit = sum(reach for _, reach in found)
            at = [pl.ds((2 * slot + part) * width, width) for part in range(2)]

            @pl.when(number == 0)
            def _():
                for part in range(2):
                    out[top, at[part]] = jnp.zeros((height, width), BF16)

            @pl.when(number == 1)
            def _():
                for part in range(2):
                    out[top, at[part]] = masked(held[c, which, part], rows, cols, limit).astype(BF16)

            @pl.when(number > 1)
            def _():
                for part in range(2):
                    total = jnp.zeros((height, width), F32)
                    for q in range(slots):
                        total = total + masked(held[c, q, part], rows, cols, found[q][1])
                    out[top, at[part]] = total.astype(BF16)


def centre_kernel(off, cnt, rng, sigma, one, two, early, late):
    slab = lax.axis_index("slab")
    step = pl.program_id(0)
    height, width = sigma.shape[-2:]
    rows, cols = index_grid(step * height, height, width)
    found = matches(slab, 0, off, cnt, rng)
    for part in range(2):
        mixed = 0.5 * (one[0, 0, part].astype(F32) + two[0, 0, part].astype(F32))
        total = mixed.astype(BF16).astype(F32)
        for q in range(sigma.shape[2]):
            total = total + masked(sigma[0, 0, q, part], rows, cols, found[q][1])
        at = pl.ds(part * width, width)

        @pl.when(step < SPLIT // height)
        def _():
            early[pl.ds(pl.multiple_of(step * height, height), height), at] = total.astype(BF16)

        @pl.when(step >= SPLIT // height)
        def _():
            below = pl.multiple_of(step * height - SPLIT, height)
            late[pl.ds(below, height), at] = total.astype(BF16)


def green_kernel(green, right, left, left_early, left_late):
    width = green.shape[-1]
    s = toward()
    for slot, o in enumerate((1 + s, 1, 1 - s)):
        real, imag = green[0, 0, o, 0], green[0, 0, o, 1]
        real_t, imag_t = real.T, imag.T
        at = 2 * slot * width
        right[at : at + width, :width] = real_t
        right[at : at + width, width:] = -imag_t
        right[at + width : at + 2 * width, :width] = imag_t
        right[at + width : at + 2 * width, width:] = real_t
        if slot == 1:
            left[:, :width] = real
            left[:, width:] = imag
        else:
            for out, first, last in ((left_early, 0, SPLIT), (left_late, SPLIT, width)):
                height = last - first
                to = slot * height
                out[:, to : to + height] = real[:, first:last]
                out[:, to + height : to + 2 * height] = imag[:, first:last]


def spread(x, out, first):
    height, width = x.shape[0], x.shape[1] // 2
    rounded = x.astype(BF16)
    real, imag = rounded[:, :width], rounded[:, width:]
    out[first : first + height, :width] = real
    out[first : first + height, width:] = imag
    out[first + height : first + 2 * height, :width] = -imag
    out[first + height : first + 2 * height, width:] = real


def local_kernel(first, early, late, second, right, left, out, held):
    wide = early.shape[1]
    x = dot(first[:, :wide], right[:wide]) + dot(second[:, wide:], right[2 * wide :])
    middle = right[wide : 2 * wide]
    x = x + jnp.concatenate([dot(early[...], middle), dot(late[...], middle)], axis=0)
    spread(x, held, 0)
    out[...] = dot(left[...], held[...])


def arrive_kernel(from_first, from_second, right, out_first, out_second):
    wide = out_first.shape[1]
    out_first[...] = dot(from_first[...], right[wide:])
    out_second[...] = dot(from_second[...], right[: 2 * wide])


def fold(c_first, c_second, x_first, x_second, right, held, first):
    height, wide = c_first.shape
    top = slice(first, first + height)
    spread(x_first[top, :] + dot(c_first[...], right[:wide]), held, 0)
    spread(x_second[top, :] + dot(c_second[...], right[2 * wide :]), held, 2 * height)


def early_kernel(c_first, c_second, x_first, x_second, right, left, partial, out, held):
    fold(c_first, c_second, x_first, x_second, right, held, 0)
    out[...] = partial[...] + dot(left[...], held[...])


def late_kernel(c_first, c_second, x_first, x_second, right, left, partial, out, held, stage, sems):
    width = stage.shape[-1]
    fold(c_first, c_second, x_first, x_second, right, held, SPLIT)
    height = width // CHUNKS
    copies = []
    for c in range(CHUNKS):
        top = pl.ds(c * height, height)
        total = partial[top, :] + dot(left[top, :], held[...])
        stage[0, top, :] = total[:, :width]
        stage[1, top, :] = total[:, width:]
        copies.append(
            pltpu.make_async_copy(stage.at[:, top, :], out.at[0, 0, :, top, :], sems.at[c])
        )
        copies[-1].start()
    for copy in copies:
        copy.wait()


def smem():
    return pl.BlockSpec(memory_space=pltpu.SMEM)


def hbm():
    return pl.BlockSpec(memory_space=pltpu.HBM)


def params():
    return pltpu.CompilerParams(vmem_limit_bytes=VMEM_LIMIT)


def swaps(first, count):
    pairs = []
    for i in range(first, count - 1, 2):
        pairs += [(i, i + 1), (i + 1, i)]
    return pairs


def swap(value, axis, first):
    return lax.ppermute(value, axis, swaps(first, lax.axis_size(axis)))


def in_hbm(value):
    return pltpu.with_memory_space_constraint(value, pltpu.HBM)


def program(green, sigma, phonon, pair_off, pair_count, pair_range):
    width = green.shape[-1]
    wide = 2 * width
    slots = sigma.shape[2]
    tables = (pair_off.T, pair_count, pair_range.T)
    block_bytes = 2 * width * wide
    height = width // CHUNKS

    first, second = pl.pallas_call(
        side_kernel,
        in_specs=[hbm()] * 4,
        out_shape=[jax.ShapeDtypeStruct((width, 2 * wide), BF16)] * 2,
        scratch_shapes=[
            pltpu.SMEM(tables[0].shape, jnp.int32),
            pltpu.SMEM(tables[1].shape, jnp.int32),
            pltpu.SMEM(tables[2].shape, jnp.int32),
            pltpu.VMEM((CHUNKS, slots, 2, height, width), BF16),
            pltpu.SemaphoreType.DMA((CHUNKS,)),
            pltpu.SemaphoreType.DMA((3,)),
        ],
        compiler_params=params(),
        cost_estimate=cost(3e9, 7 * block_bytes),
        name="side",
    )(*[in_hbm(value) for value in (*tables, sigma)])
    from_first = swap(first, "slab", 0)
    from_second = swap(second, "slab", 1)

    one = swap(phonon, "energy", 0)
    two = swap(phonon, "energy", 1)

    sigma_spec = pl.BlockSpec((1, 1, slots, 2, height, width), lambda c: (0, 0, 0, 0, c, 0))
    phonon_spec = pl.BlockSpec((1, 1, 2, height, width), lambda c: (0, 0, 0, c, 0))
    whole = lambda rows: pl.BlockSpec((rows, wide), lambda c: (0, 0))
    early, late = pl.pallas_call(
        centre_kernel,
        grid=(CHUNKS,),
        in_specs=[smem(), smem(), smem(), sigma_spec, phonon_spec, phonon_spec],
        out_specs=[whole(SPLIT), whole(width - SPLIT)],
        out_shape=[
            jax.ShapeDtypeStruct((SPLIT, wide), BF16),
            jax.ShapeDtypeStruct((width - SPLIT, wide), BF16),
        ],
        compiler_params=params(),
        cost_estimate=cost(3e9, 6 * block_bytes),
        name="centre",
    )(*[in_hbm(value) for value in (*tables, sigma)], one, two)
    early_second = swap(early, "slab", 1)
    early_first = swap(early, "slab", 0)
    late_second = swap(late, "slab", 1)
    late_first = swap(late, "slab", 0)

    right, left, left_early, left_late = pl.pallas_call(
        green_kernel,
        out_shape=[
            jax.ShapeDtypeStruct((3 * wide, wide), BF16),
            jax.ShapeDtypeStruct((width, wide), BF16),
            jax.ShapeDtypeStruct((width, 4 * SPLIT), BF16),
            jax.ShapeDtypeStruct((width, 4 * (width - SPLIT)), BF16),
        ],
        compiler_params=params(),
        cost_estimate=cost(4e9, 12 * block_bytes),
        name="green",
    )(in_hbm(green))

    square = jax.ShapeDtypeStruct((width, wide), F32)
    unit = 2 * width * wide * wide
    partial = pl.pallas_call(
        local_kernel,
        out_shape=square,
        scratch_shapes=[pltpu.VMEM((wide, wide), BF16)],
        compiler_params=params(),
        cost_estimate=cost(4 * unit, 16 * block_bytes),
        name="local",
    )(first, early, late, second, right, left)

    x_first, x_second = pl.pallas_call(
        arrive_kernel,
        out_shape=[square, square],
        compiler_params=params(),
        cost_estimate=cost(4 * unit, 16 * block_bytes),
        name="arrive",
    )(from_first, from_second, right)

    partial = pl.pallas_call(
        early_kernel,
        out_shape=square,
        scratch_shapes=[pltpu.VMEM((4 * SPLIT, wide), BF16)],
        compiler_params=params(),
        cost_estimate=cost(3 * unit, 16 * block_bytes),
        name="early",
    )(early_first, early_second, x_first, x_second, right, left_early, partial)

    return pl.pallas_call(
        late_kernel,
        out_specs=hbm(),
        out_shape=jax.ShapeDtypeStruct((1, 1, 2, width, width), F32),
        scratch_shapes=[
            pltpu.VMEM((4 * (width - SPLIT), wide), BF16),
            pltpu.VMEM((2, width, width), F32),
            pltpu.SemaphoreType.DMA((CHUNKS,)),
        ],
        compiler_params=params(),
        cost_estimate=cost(2 * unit, 16 * block_bytes),
        name="late",
    )(late_first, late_second, x_first, x_second, right, left_late, partial)


def solution(mesh):
    in_specs = (
        P("energy", "slab", None, None, None, None),
        P("energy", "slab", None, None, None, None),
        P("energy", "slab", None, None, None),
        P(),
        P(),
        P(),
    )
    out_specs = P("energy", "slab", None, None, None)
    return jax.shard_map(program, mesh=mesh, in_specs=in_specs, out_specs=out_specs, check_vma=False)
```

```python
import functools

import jax
import jax.numpy as jnp
from jax import lax
from jax.experimental import pallas as pl
from jax.experimental.pallas import tpu as pltpu
from jax.sharding import PartitionSpec as P


F32 = jnp.float32
BF16 = jnp.bfloat16
VMEM_LIMIT = 24 * 1024 * 1024
CHUNKS = 3
PIECE = 48
LEVELS = (192, 288, 384)
SPLIT = 256


def cost(flops, moved):
    return pl.CostEstimate(flops=int(flops), bytes_accessed=int(moved), transcendentals=0)


def dot(left, right):
    return jnp.dot(left, right, preferred_element_type=F32)


def toward():
    return 1 - 2 * lax.rem(lax.axis_index("slab"), 2)


def matches(slab, offset, off, cnt, rng):
    found = []
    for q in range(off.shape[0]):
        live = (off[q, slab] == offset) & (q < cnt[slab])
        found.append((live.astype(jnp.int32), jnp.where(live, rng[q, slab], 0)))
    return found


def masked(block, rows, cols, limit):
    return jnp.where((rows < limit) & (cols < limit), block.astype(F32), 0.0)


def index_grid(first, height, width):
    rows = lax.broadcasted_iota(jnp.int32, (height, width), 0) + first
    cols = lax.broadcasted_iota(jnp.int32, (height, width), 1)
    return rows, cols


def packing(reach, width):
    if reach == width:
        return 2 * width, width, 0
    body = reach // 128 * 128
    groups = 2 * body // 128 + 1
    lanes = 2 * width // 128
    return width + groups * (reach // PIECE) // lanes * PIECE, body, reach - body


def unit_at(group, piece, reach, width):
    lanes = 2 * width // 128
    unit = group * (reach // PIECE) + piece
    return width + unit // lanes * PIECE, unit % lanes * 128


def widest_small(off, cnt, rng):
    slots = lax.broadcasted_iota(jnp.int32, off.shape, 0)
    live = slots < cnt[...]

    def reach(offset):
        return jnp.max(jnp.where(live & (off[...] == offset), rng[...], 0), axis=0, keepdims=True)

    low = jnp.minimum(reach(-1), reach(-2))
    high = jnp.minimum(reach(1), reach(2))
    return jnp.max(jnp.maximum(low, high))


def near_leads(slab, d, off, cnt, rng):
    near, far = [
        functools.reduce(jnp.maximum, [reach for _, reach in matches(slab, offset, off, cnt, rng)])
        for offset in (d, 2 * d)
    ]
    return near >= far


def side_kernel(off_in, cnt_in, rng_in, sigma, *refs):
    outs, (level, roles) = refs[: 2 * len(LEVELS)], refs[2 * len(LEVELS) : 2 * len(LEVELS) + 2]
    off, cnt, rng, off_v, cnt_v, rng_v, held, sems, table_sems = refs[2 * len(LEVELS) + 2 :]
    slab = lax.axis_index("slab")
    s = toward()
    chunks, slots, _, height, width = held.shape
    moves = (
        (off_in, off_v),
        (cnt_in, cnt_v),
        (rng_in, rng_v),
        (off_in, off),
        (cnt_in, cnt),
        (rng_in, rng),
    )
    tables = [
        pltpu.make_async_copy(src, dst, table_sems.at[n]) for n, (src, dst) in enumerate(moves)
    ]
    copies = [
        pltpu.make_async_copy(
            sigma.at[0, 0, :, :, pl.ds(c * height, height), :], held.at[c], sems.at[c]
        )
        for c in range(chunks)
    ]
    for copy in tables + copies:
        copy.start()
    for copy in tables:
        copy.wait()
    widest = widest_small(off_v, cnt_v, rng_v)
    rank = sum((widest > reach).astype(jnp.int32) for reach in LEVELS[:-1])
    level[0] = rank
    cnt = cnt.at[0]
    last = off.shape[1] - 1
    for n, d in enumerate((s, -s)):
        neighbour = jnp.clip(slab + d, 0, last)
        roles[n] = near_leads(neighbour, -d, off, cnt, rng).astype(jnp.int32)

    merges, messages = [], []
    for d in (s, -s):
        sides = []
        for offset in (d, 2 * d):
            found = matches(slab, offset, off, cnt, rng)
            number = sum(live for live, _ in found)
            which = jnp.int32(0)
            for q in reversed(range(slots)):
                which = jnp.where(found[q][0] > 0, q, which)
            reach = functools.reduce(jnp.maximum, [reach for _, reach in found])
            merges.append((number, which, [reach for _, reach in found]))
            sides.append((which, reach))
        near, far = sides
        leads = near[1] >= far[1]
        big = tuple(jnp.where(leads, u, v) for u, v in zip(near, far))
        small = tuple(jnp.where(leads, v, u) for u, v in zip(near, far))
        messages.append((big, small))

    for c in range(chunks):
        copies[c].wait()
        rows, cols = index_grid(c * height, height, width)
        for number, which, reaches in merges:

            @pl.when(number > 1)
            def _():
                for part in range(2):
                    total = jnp.zeros((height, width), F32)
                    for q in range(slots):
                        total = total + masked(held[c, q, part], rows, cols, reaches[q])
                    held[c, which, part] = total.astype(BF16)

        for n, (big, small) in enumerate(messages):
            for index, reach in enumerate(LEVELS):
                out = outs[2 * index + n]

                @pl.when(rank == index)
                def _():
                    for part in range(2):
                        block = masked(held[c, big[0], part], rows, cols, big[1])
                        out[c * height : (c + 1) * height, part * width : (part + 1) * width] = (
                            block.astype(BF16)
                        )
                    _, body, rest = packing(reach, width)
                    if rest == 0:
                        for part in range(2):
                            block = masked(held[c, small[0], part], rows, cols, small[1])
                            first = width + c * height
                            out[first : first + height, part * width : (part + 1) * width] = (
                                block.astype(BF16)
                            )
                        return
                    for piece in range(c * height // PIECE, (c + 1) * height // PIECE):
                        if piece >= reach // PIECE:
                            continue
                        first = piece * PIECE - c * height
                        inner = slice(first, first + PIECE)
                        parts = [
                            masked(
                                held[c, small[0], part, inner, : body + 128],
                                rows[inner, : body + 128],
                                cols[inner, : body + 128],
                                small[1],
                            )
                            for part in range(2)
                        ]
                        units = [part[:, at : at + 128] for part in parts for at in range(0, body, 128)]
                        units.append(parts[0][:, body:] + pltpu.roll(parts[1][:, body:], rest, 1))
                        for group, unit in enumerate(units):
                            row, lane = unit_at(group, piece, reach, width)
                            out[row : row + PIECE, lane : lane + 128] = unit.astype(BF16)


def centre_kernel(off, cnt, rng, sigma, one, two, early, late, near_first, near_second):
    slab = lax.axis_index("slab")
    cnt = cnt.at[0]
    step = pl.program_id(0)
    height, width = sigma.shape[-2:]
    rows, cols = index_grid(step * height, height, width)
    found = matches(slab, 0, off, cnt, rng)
    for part in range(2):
        mixed = 0.5 * (one[0, 0, part].astype(F32) + two[0, 0, part].astype(F32))
        total = mixed.astype(BF16).astype(F32)
        for q in range(sigma.shape[2]):
            total = total + masked(sigma[0, 0, q, part], rows, cols, found[q][1])
        at = pl.ds(part * width, width)
        for d, out in ((toward(), near_first), (-toward(), near_second)):
            near = jnp.zeros((height, width), F32)
            for q, (_, reach) in enumerate(matches(slab, d, off, cnt, rng)):
                near = near + masked(sigma[0, 0, q, part], rows, cols, reach)
            out[:, at] = near.astype(BF16)

        @pl.when(step < SPLIT // height)
        def _():
            early[pl.ds(pl.multiple_of(step * height, height), height), at] = total.astype(BF16)

        @pl.when(step >= SPLIT // height)
        def _():
            below = pl.multiple_of(step * height - SPLIT, height)
            late[pl.ds(below, height), at] = total.astype(BF16)


def green_kernel(green, right, left, left_early, left_late):
    width = green.shape[-1]
    s = toward()
    for slot, o in enumerate((1 + s, 1, 1 - s)):
        real, imag = green[0, 0, o, 0], green[0, 0, o, 1]
        real_t, imag_t = real.T, imag.T
        at = 2 * slot * width
        right[at : at + width, :width] = real_t
        right[at : at + width, width:] = -imag_t
        right[at + width : at + 2 * width, :width] = imag_t
        right[at + width : at + 2 * width, width:] = real_t
        if slot == 1:
            left[:, :width] = real
            left[:, width:] = imag
        else:
            for out, first, last in ((left_early, 0, SPLIT), (left_late, SPLIT, width)):
                height = last - first
                to = slot * height
                out[:, to : to + height] = real[:, first:last]
                out[:, to + height : to + 2 * height] = imag[:, first:last]


def spread(x, out, first):
    height, width = x.shape[0], x.shape[1] // 2
    rounded = x.astype(BF16)
    real, imag = rounded[:, :width], rounded[:, width:]
    out[first : first + height, :width] = real
    out[first : first + height, width:] = imag
    out[first + height : first + 2 * height, :width] = -imag
    out[first + height : first + 2 * height, width:] = real


def local_kernel(near_first, early, late, near_second, right, left, out, held):
    wide = early.shape[1]
    x = dot(near_first[...], right[:wide]) + dot(near_second[...], right[2 * wide :])
    middle = right[wide : 2 * wide]
    x = x + jnp.concatenate([dot(early[...], middle), dot(late[...], middle)], axis=0)
    spread(x, held, 0)
    out[...] = dot(left[...], held[...])


def arrive_kernel(reach, roles, from_first, from_second, right, out_first, out_second, *packed):
    width, wide = out_first.shape
    for n, (message, out, other) in enumerate(
        ((from_first, out_first, 2 * wide), (from_second, out_second, 0))
    ):
        leads = roles[n] > 0
        big_at = pl.multiple_of(jnp.where(leads, wide, other), wide)
        small_at = pl.multiple_of(jnp.where(leads, other, wide), wide)
        total = dot(message[:width], right[pl.ds(big_at, wide)])
        if reach == width:
            out[...] = total + dot(message[width:], right[pl.ds(small_at, wide)])
            continue
        left, down = packed
        _, body, rest = packing(reach, width)
        for group in range(2 * body // 128 + 1):
            for piece in range(reach // PIECE):
                row, lane = unit_at(group, piece, reach, width)
                left[piece * PIECE : (piece + 1) * PIECE, group * 128 : (group + 1) * 128] = (
                    message[row : row + PIECE, lane : lane + 128]
                )
        for part in range(2):
            source = pl.multiple_of(small_at + part * width, width)
            down[part * body : (part + 1) * body] = right[pl.ds(source, body)]
            tail = pl.multiple_of(small_at + part * width + body, 128)
            to = 2 * body + part * rest
            down[to : to + rest] = right[pl.ds(tail, rest)]
        if 2 * rest < 128:
            down[2 * body + 2 * rest :] = jnp.zeros((128 - 2 * rest, wide), BF16)
        out[:reach] = total[:reach] + dot(left[...], down[...])
        out[reach:] = total[reach:]


def fold(c_first, c_second, x_first, x_second, right, held, first):
    height, wide = c_first.shape
    top = slice(first, first + height)
    spread(x_first[top, :] + dot(c_first[...], right[:wide]), held, 0)
    spread(x_second[top, :] + dot(c_second[...], right[2 * wide :]), held, 2 * height)


def early_kernel(c_first, c_second, x_first, x_second, right, left, partial, out, held):
    fold(c_first, c_second, x_first, x_second, right, held, 0)
    out[...] = partial[...] + dot(left[...], held[...])


def late_kernel(c_first, c_second, x_first, x_second, right, left, partial, out, held, stage, sems):
    width = stage.shape[-1]
    fold(c_first, c_second, x_first, x_second, right, held, SPLIT)
    height = width // CHUNKS
    copies = []
    for c in range(CHUNKS):
        top = pl.ds(c * height, height)
        total = partial[top, :] + dot(left[top, :], held[...])
        stage[0, top, :] = total[:, :width]
        stage[1, top, :] = total[:, width:]
        copies.append(
            pltpu.make_async_copy(stage.at[:, top, :], out.at[0, 0, :, top, :], sems.at[c])
        )
        copies[-1].start()
    for copy in copies:
        copy.wait()


def smem():
    return pl.BlockSpec(memory_space=pltpu.SMEM)


def hbm():
    return pl.BlockSpec(memory_space=pltpu.HBM)


def params():
    return pltpu.CompilerParams(vmem_limit_bytes=VMEM_LIMIT)


def swaps(first, count):
    pairs = []
    for i in range(first, count - 1, 2):
        pairs += [(i, i + 1), (i + 1, i)]
    return pairs


def swap(value, axis, first):
    return lax.ppermute(value, axis, swaps(first, lax.axis_size(axis)))


def in_hbm(value):
    return pltpu.with_memory_space_constraint(value, pltpu.HBM)


def program(green, sigma, phonon, pair_off, pair_count, pair_range):
    width = green.shape[-1]
    wide = 2 * width
    slots = sigma.shape[2]
    tables = (pair_off.T, pair_count[None], pair_range.T)
    block_bytes = 2 * width * wide
    chunks = width // (2 * PIECE)

    messages = []
    for reach in LEVELS:
        rows = packing(reach, width)[0]
        messages += [jax.ShapeDtypeStruct((rows, wide), BF16)] * 2
    *messages, level, roles = pl.pallas_call(
        side_kernel,
        in_specs=[hbm()] * 4,
        out_specs=[pl.BlockSpec(memory_space=pltpu.VMEM)] * len(messages) + [smem(), smem()],
        out_shape=[
            *messages,
            jax.ShapeDtypeStruct((1,), jnp.int32),
            jax.ShapeDtypeStruct((2,), jnp.int32),
        ],
        scratch_shapes=[
            *[pltpu.SMEM(table.shape, jnp.int32) for table in tables],
            *[pltpu.VMEM(table.shape, jnp.int32) for table in tables],
            pltpu.VMEM((chunks, slots, 2, 2 * PIECE, width), BF16),
            pltpu.SemaphoreType.DMA((chunks,)),
            pltpu.SemaphoreType.DMA((6,)),
        ],
        compiler_params=params(),
        cost_estimate=cost(3e9, 7 * block_bytes),
        name="side",
    )(*[in_hbm(value) for value in (*tables, sigma)])
    branches = [functools.partial(remainder, reach, 2 * n) for n, reach in enumerate(LEVELS)]
    return lax.switch(level[0], branches, messages, roles, green, sigma, phonon, tables)


def remainder(reach, index, messages, roles, green, sigma, phonon, tables):
    first, second = messages[index : index + 2]
    width = green.shape[-1]
    wide = 2 * width
    slots = sigma.shape[2]
    block_bytes = 2 * width * wide
    height = width // CHUNKS
    from_first = swap(first, "slab", 0)
    from_second = swap(second, "slab", 1)

    one = swap(phonon, "energy", 0)
    two = swap(phonon, "energy", 1)

    sigma_spec = pl.BlockSpec((1, 1, slots, 2, height, width), lambda c: (0, 0, 0, 0, c, 0))
    phonon_spec = pl.BlockSpec((1, 1, 2, height, width), lambda c: (0, 0, 0, c, 0))
    whole = lambda rows: pl.BlockSpec((rows, wide), lambda c: (0, 0))
    chunk = pl.BlockSpec((height, wide), lambda c: (c, 0))
    early, late, near_first, near_second = pl.pallas_call(
        centre_kernel,
        grid=(CHUNKS,),
        in_specs=[smem(), smem(), smem(), sigma_spec, phonon_spec, phonon_spec],
        out_specs=[whole(SPLIT), whole(width - SPLIT), chunk, chunk],
        out_shape=[
            jax.ShapeDtypeStruct((SPLIT, wide), BF16),
            jax.ShapeDtypeStruct((width - SPLIT, wide), BF16),
            jax.ShapeDtypeStruct((width, wide), BF16),
            jax.ShapeDtypeStruct((width, wide), BF16),
        ],
        compiler_params=params(),
        cost_estimate=cost(3e9, 6 * block_bytes),
        name="centre",
    )(*[in_hbm(value) for value in (*tables, sigma)], one, two)
    early_second = swap(early, "slab", 1)
    early_first = swap(early, "slab", 0)
    late_second = swap(late, "slab", 1)
    late_first = swap(late, "slab", 0)

    right, left, left_early, left_late = pl.pallas_call(
        green_kernel,
        out_shape=[
            jax.ShapeDtypeStruct((3 * wide, wide), BF16),
            jax.ShapeDtypeStruct((width, wide), BF16),
            jax.ShapeDtypeStruct((width, 4 * SPLIT), BF16),
            jax.ShapeDtypeStruct((width, 4 * (width - SPLIT)), BF16),
        ],
        compiler_params=params(),
        cost_estimate=cost(4e9, 12 * block_bytes),
        name="green",
    )(in_hbm(green))

    square = jax.ShapeDtypeStruct((width, wide), F32)
    unit = 2 * width * wide * wide
    partial = pl.pallas_call(
        local_kernel,
        out_shape=square,
        scratch_shapes=[pltpu.VMEM((wide, wide), BF16)],
        compiler_params=params(),
        cost_estimate=cost(4 * unit, 16 * block_bytes),
        name="local",
    )(near_first, early, late, near_second, right, left)

    _, body, rest = packing(reach, width)
    depth = 2 * body + 128
    packed = [pltpu.VMEM((reach, depth), BF16), pltpu.VMEM((depth, wide), BF16)]
    x_first, x_second = pl.pallas_call(
        functools.partial(arrive_kernel, reach),
        in_specs=[smem()] + [pl.BlockSpec(memory_space=pltpu.VMEM)] * 3,
        out_shape=[square, square],
        scratch_shapes=packed if rest else [],
        compiler_params=params(),
        cost_estimate=cost(4 * unit, 16 * block_bytes),
        name="arrive",
    )(roles, from_first, from_second, right)

    partial = pl.pallas_call(
        early_kernel,
        out_shape=square,
        scratch_shapes=[pltpu.VMEM((4 * SPLIT, wide), BF16)],
        compiler_params=params(),
        cost_estimate=cost(3 * unit, 16 * block_bytes),
        name="early",
    )(early_first, early_second, x_first, x_second, right, left_early, partial)

    return pl.pallas_call(
        late_kernel,
        out_specs=hbm(),
        out_shape=pltpu.HBM((1, 1, 2, width, width), F32),
        scratch_shapes=[
            pltpu.VMEM((4 * (width - SPLIT), wide), BF16),
            pltpu.VMEM((2, width, width), F32),
            pltpu.SemaphoreType.DMA((CHUNKS,)),
        ],
        compiler_params=params(),
        cost_estimate=cost(2 * unit, 16 * block_bytes),
        name="late",
    )(late_first, late_second, x_first, x_second, right, left_late, partial)


def solution(mesh):
    in_specs = (
        P("energy", "slab", None, None, None, None),
        P("energy", "slab", None, None, None, None),
        P("energy", "slab", None, None, None),
        P(),
        P(),
        P(),
    )
    out_specs = P("energy", "slab", None, None, None)
    return jax.shard_map(program, mesh=mesh, in_specs=in_specs, out_specs=out_specs, check_vma=False)
```

```python
import functools

import jax
import jax.numpy as jnp
from jax import lax
from jax.experimental import pallas as pl
from jax.experimental.pallas import tpu as pltpu
from jax.sharding import PartitionSpec as P


F32 = jnp.float32
BF16 = jnp.bfloat16
VMEM_LIMIT = 24 * 1024 * 1024
CHUNKS = 3
PIECE = 48
LEVELS = (192, 288, 384)
SPLIT = 256


def cost(flops, moved):
    return pl.CostEstimate(flops=int(flops), bytes_accessed=int(moved), transcendentals=0)


def dot(left, right):
    return jnp.dot(left, right, preferred_element_type=F32)


def toward():
    return 1 - 2 * lax.rem(lax.axis_index("slab"), 2)


def matches(slab, offset, off, cnt, rng):
    found = []
    for q in range(off.shape[0]):
        live = (off[q, slab] == offset) & (q < cnt[slab])
        found.append((live.astype(jnp.int32), jnp.where(live, rng[q, slab], 0)))
    return found


def inside(lanes, reach, first):
    return (lanes < jnp.where(first < reach, reach, 0)).astype(F32).astype(BF16)


def strip_sum(sigma, part, reaches, lanes, c):
    slots, _, height, width = sigma.shape
    total = jnp.zeros((height, width), F32)
    for q in range(slots):
        total = total + (sigma[q, part] * inside(lanes, reaches[q], c * height)).astype(F32)
    return total


def packing(reach, width):
    if reach == width:
        return 2 * width, width, 0
    body = reach // 128 * 128
    groups = 2 * body // 128 + 1
    lanes = 2 * width // 128
    return width + groups * (reach // PIECE) // lanes * PIECE, body, reach - body


def unit_at(group, piece, reach, width):
    lanes = 2 * width // 128
    unit = group * (reach // PIECE) + piece
    return width + unit // lanes * PIECE, unit % lanes * 128


def widest_small(off, cnt, rng):
    slots = lax.broadcasted_iota(jnp.int32, off.shape, 0)
    live = slots < cnt[...]

    def reach(offset):
        return jnp.max(jnp.where(live & (off[...] == offset), rng[...], 0), axis=0, keepdims=True)

    low = jnp.minimum(reach(-1), reach(-2))
    high = jnp.minimum(reach(1), reach(2))
    return jnp.max(jnp.maximum(low, high))


def near_leads(slab, d, off, cnt, rng):
    near, far = [
        functools.reduce(jnp.maximum, [reach for _, reach in matches(slab, offset, off, cnt, rng)])
        for offset in (d, 2 * d)
    ]
    return near >= far


def side_kernel(off_in, cnt_in, rng_in, sigma, *refs):
    outs, (level, roles) = refs[: 2 * len(LEVELS)], refs[2 * len(LEVELS) : 2 * len(LEVELS) + 2]
    off, cnt, rng, off_v, cnt_v, rng_v, held, sems, table_sems = refs[2 * len(LEVELS) + 2 :]
    slab = lax.axis_index("slab")
    s = toward()
    chunks, slots, _, height, width = held.shape
    moves = (
        (off_in, off_v),
        (cnt_in, cnt_v),
        (rng_in, rng_v),
        (off_in, off),
        (cnt_in, cnt),
        (rng_in, rng),
    )
    tables = [
        pltpu.make_async_copy(src, dst, table_sems.at[n]) for n, (src, dst) in enumerate(moves)
    ]
    copies = [
        pltpu.make_async_copy(
            sigma.at[0, 0, :, :, pl.ds(c * height, height), :], held.at[c], sems.at[c]
        )
        for c in range(chunks)
    ]
    for copy in tables + copies:
        copy.start()
    for copy in tables:
        copy.wait()
    widest = widest_small(off_v, cnt_v, rng_v)
    rank = sum((widest > reach).astype(jnp.int32) for reach in LEVELS[:-1])
    level[0] = rank
    cnt = cnt.at[0]
    last = off.shape[1] - 1
    for n, d in enumerate((s, -s)):
        neighbour = jnp.clip(slab + d, 0, last)
        roles[n] = near_leads(neighbour, -d, off, cnt, rng).astype(jnp.int32)

    merges, messages = [], []
    for d in (s, -s):
        sides = []
        for offset in (d, 2 * d):
            found = matches(slab, offset, off, cnt, rng)
            number = sum(live for live, _ in found)
            which = jnp.int32(0)
            for q in reversed(range(slots)):
                which = jnp.where(found[q][0] > 0, q, which)
            reach = functools.reduce(jnp.maximum, [reach for _, reach in found])
            merges.append((number, which, [reach for _, reach in found]))
            sides.append((which, reach))
        near, far = sides
        leads = near[1] >= far[1]
        big = tuple(jnp.where(leads, u, v) for u, v in zip(near, far))
        small = tuple(jnp.where(leads, v, u) for u, v in zip(near, far))
        messages.append((big, small))

    lanes = lax.broadcasted_iota(jnp.int32, (1, width), 1)
    for c in range(chunks):
        copies[c].wait()
        rows = slice(c * height, (c + 1) * height)
        for number, which, reaches in merges:

            @pl.when(number > 1)
            def _():
                for part in range(2):
                    held[c, which, part] = strip_sum(held.at[c], part, reaches, lanes, c).astype(BF16)

        for n, (big, small) in enumerate(messages):
            keep_big = inside(lanes, big[1], c * height)
            keep_small = inside(lanes, small[1], c * height)
            for index, reach in enumerate(LEVELS):
                out = outs[2 * index + n]

                @pl.when(rank == index)
                def _():
                    for part in range(2):
                        to = slice(part * width, (part + 1) * width)
                        out[rows, to] = held[c, big[0], part] * keep_big
                    _, body, rest = packing(reach, width)
                    if rest == 0:
                        for part in range(2):
                            to = slice(part * width, (part + 1) * width)
                            first = width + c * height
                            out[first : first + height, to] = held[c, small[0], part] * keep_small
                        return
                    if c * height >= reach:
                        return
                    parts = [
                        held[c, small[0], part, :, : body + 128] * keep_small[:, : body + 128]
                        for part in range(2)
                    ]
                    tail = parts[0][:, body:].astype(F32)
                    tail = tail + pltpu.roll(parts[1][:, body:].astype(F32), rest, 1)
                    units = [part[:, at : at + 128] for part in parts for at in range(0, body, 128)]
                    units.append(tail.astype(BF16))
                    for group, unit in enumerate(units):
                        for half in range(2):
                            row, lane = unit_at(group, 2 * c + half, reach, width)
                            out[row : row + PIECE, lane : lane + 128] = unit[
                                half * PIECE : (half + 1) * PIECE
                            ]


def own_kernel(off, cnt, rng, sigma, near_first, near_second, middle):
    slab = lax.axis_index("slab")
    cnt = cnt.at[0]
    _, _, _, width = sigma.shape[2:]
    lanes = lax.broadcasted_iota(jnp.int32, (1, width), 1)
    c = pl.program_id(0)
    for offset, out in ((toward(), near_first), (-toward(), near_second), (0, middle)):
        reaches = [reach for _, reach in matches(slab, offset, off, cnt, rng)]
        for part in range(2):
            total = strip_sum(sigma.at[0, 0], part, reaches, lanes, c)
            out[:, part * width : (part + 1) * width] = total.astype(out.dtype)


def centre_kernel(middle, one, two, early, late):
    width = middle.shape[1] // 2
    for part in range(2):
        mixed = 0.5 * (one[0, 0, part].astype(F32) + two[0, 0, part].astype(F32))
        at = slice(part * width, (part + 1) * width)
        total = (middle[:, at] + mixed.astype(BF16).astype(F32)).astype(BF16)
        early[:, at] = total[:SPLIT]
        late[:, at] = total[SPLIT:]


def green_kernel(green, right, left, left_early, left_late):
    width = green.shape[-1]
    s = toward()
    for slot, o in enumerate((1 + s, 1, 1 - s)):
        real, imag = green[0, 0, o, 0], green[0, 0, o, 1]
        real_t, imag_t = real.T, imag.T
        at = 2 * slot * width
        right[at : at + width, :width] = real_t
        right[at : at + width, width:] = -imag_t
        right[at + width : at + 2 * width, :width] = imag_t
        right[at + width : at + 2 * width, width:] = real_t
        if slot == 1:
            left[:, :width] = real
            left[:, width:] = imag
        else:
            for out, first, last in ((left_early, 0, SPLIT), (left_late, SPLIT, width)):
                height = last - first
                to = slot * height
                out[:, to : to + height] = real[:, first:last]
                out[:, to + height : to + 2 * height] = imag[:, first:last]


def spread(x, out, first):
    height, width = x.shape[0], x.shape[1] // 2
    rounded = x.astype(BF16)
    real, imag = rounded[:, :width], rounded[:, width:]
    out[first : first + height, :width] = real
    out[first : first + height, width:] = imag
    out[first + height : first + 2 * height, :width] = -imag
    out[first + height : first + 2 * height, width:] = real


def local_kernel(near_first, early, late, near_second, right, left, out, held):
    wide = early.shape[1]
    x = dot(near_first[...], right[:wide]) + dot(near_second[...], right[2 * wide :])
    middle = right[wide : 2 * wide]
    x = x + jnp.concatenate([dot(early[...], middle), dot(late[...], middle)], axis=0)
    spread(x, held, 0)
    out[...] = dot(left[...], held[...])


def arrive_kernel(reach, roles, from_first, from_second, right, out_first, out_second, *packed):
    width, wide = out_first.shape
    for n, (message, out, other) in enumerate(
        ((from_first, out_first, 2 * wide), (from_second, out_second, 0))
    ):
        leads = roles[n] > 0
        big_at = pl.multiple_of(jnp.where(leads, wide, other), wide)
        small_at = pl.multiple_of(jnp.where(leads, other, wide), wide)
        total = dot(message[:width], right[pl.ds(big_at, wide)])
        if reach == width:
            out[...] = total + dot(message[width:], right[pl.ds(small_at, wide)])
            continue
        left, down = packed
        _, body, rest = packing(reach, width)
        for group in range(2 * body // 128 + 1):
            for piece in range(reach // PIECE):
                row, lane = unit_at(group, piece, reach, width)
                left[piece * PIECE : (piece + 1) * PIECE, group * 128 : (group + 1) * 128] = (
                    message[row : row + PIECE, lane : lane + 128]
                )
        for part in range(2):
            source = pl.multiple_of(small_at + part * width, width)
            down[part * body : (part + 1) * body] = right[pl.ds(source, body)]
            tail = pl.multiple_of(small_at + part * width + body, 128)
            to = 2 * body + part * rest
            down[to : to + rest] = right[pl.ds(tail, rest)]
        if 2 * rest < 128:
            down[2 * body + 2 * rest :] = jnp.zeros((128 - 2 * rest, wide), BF16)
        out[:reach] = total[:reach] + dot(left[...], down[...])
        out[reach:] = total[reach:]


def fold(c_first, c_second, x_first, x_second, right, held, first):
    height, wide = c_first.shape
    top = slice(first, first + height)
    spread(x_first[top, :] + dot(c_first[...], right[:wide]), held, 0)
    spread(x_second[top, :] + dot(c_second[...], right[2 * wide :]), held, 2 * height)


def early_kernel(c_first, c_second, x_first, x_second, right, left, partial, out, held):
    fold(c_first, c_second, x_first, x_second, right, held, 0)
    out[...] = partial[...] + dot(left[...], held[...])


def late_kernel(c_first, c_second, x_first, x_second, right, left, partial, out, held, stage, sems):
    width = stage.shape[-1]
    fold(c_first, c_second, x_first, x_second, right, held, SPLIT)
    height = width // CHUNKS
    copies = []
    for c in range(CHUNKS):
        top = pl.ds(c * height, height)
        total = partial[top, :] + dot(left[top, :], held[...])
        stage[0, top, :] = total[:, :width]
        stage[1, top, :] = total[:, width:]
        copies.append(
            pltpu.make_async_copy(stage.at[:, top, :], out.at[0, 0, :, top, :], sems.at[c])
        )
        copies[-1].start()
    for copy in copies:
        copy.wait()


def smem():
    return pl.BlockSpec(memory_space=pltpu.SMEM)


def hbm():
    return pl.BlockSpec(memory_space=pltpu.HBM)


def params():
    return pltpu.CompilerParams(vmem_limit_bytes=VMEM_LIMIT)


def swaps(first, count):
    pairs = []
    for i in range(first, count - 1, 2):
        pairs += [(i, i + 1), (i + 1, i)]
    return pairs


def swap(value, axis, first):
    return lax.ppermute(value, axis, swaps(first, lax.axis_size(axis)))


def in_hbm(value):
    return pltpu.with_memory_space_constraint(value, pltpu.HBM)


def program(green, sigma, phonon, pair_off, pair_count, pair_range):
    width = green.shape[-1]
    wide = 2 * width
    slots = sigma.shape[2]
    tables = (pair_off.T, pair_count[None], pair_range.T)
    block_bytes = 2 * width * wide
    chunks = width // (2 * PIECE)

    messages = []
    for reach in LEVELS:
        rows = packing(reach, width)[0]
        messages += [jax.ShapeDtypeStruct((rows, wide), BF16)] * 2
    *messages, level, roles = pl.pallas_call(
        side_kernel,
        in_specs=[hbm()] * 4,
        out_specs=[pl.BlockSpec(memory_space=pltpu.VMEM)] * len(messages) + [smem(), smem()],
        out_shape=[
            *messages,
            pltpu.SMEM((1,), jnp.int32),
            pltpu.SMEM((2,), jnp.int32),
        ],
        scratch_shapes=[
            *[pltpu.SMEM(table.shape, jnp.int32) for table in tables],
            *[pltpu.VMEM(table.shape, jnp.int32) for table in tables],
            pltpu.VMEM((chunks, slots, 2, 2 * PIECE, width), BF16),
            pltpu.SemaphoreType.DMA((chunks,)),
            pltpu.SemaphoreType.DMA((6,)),
        ],
        compiler_params=params(),
        cost_estimate=cost(3e9, 7 * block_bytes),
        name="side",
    )(*[in_hbm(value) for value in (*tables, sigma)])
    branches = [functools.partial(remainder, reach, 2 * n) for n, reach in enumerate(LEVELS)]
    return lax.switch(level[0], branches, messages, roles, green, sigma, phonon, tables)


def remainder(reach, index, messages, roles, green, sigma, phonon, tables):
    first, second = messages[index : index + 2]
    width = green.shape[-1]
    wide = 2 * width
    slots = sigma.shape[2]
    block_bytes = 2 * width * wide
    from_first = swap(first, "slab", 0)
    from_second = swap(second, "slab", 1)

    one = swap(phonon, "energy", 0)
    two = swap(phonon, "energy", 1)

    strip = 2 * PIECE
    tall = pl.BlockSpec((strip, wide), lambda c: (c, 0))
    near_first, near_second, middle = pl.pallas_call(
        own_kernel,
        grid=(width // strip,),
        in_specs=[
            *[smem()] * 3,
            pl.BlockSpec((1, 1, slots, 2, strip, width), lambda c: (0, 0, 0, 0, c, 0)),
        ],
        out_specs=[tall] * 3,
        out_shape=[
            jax.ShapeDtypeStruct((width, wide), BF16),
            jax.ShapeDtypeStruct((width, wide), BF16),
            jax.ShapeDtypeStruct((width, wide), F32),
        ],
        compiler_params=params(),
        cost_estimate=cost(3e9, 7 * block_bytes),
        name="own",
    )(*[in_hbm(value) for value in (*tables, sigma)])

    early, late = pl.pallas_call(
        centre_kernel,
        out_shape=[
            jax.ShapeDtypeStruct((SPLIT, wide), BF16),
            jax.ShapeDtypeStruct((width - SPLIT, wide), BF16),
        ],
        compiler_params=params(),
        cost_estimate=cost(1e9, 5 * block_bytes),
        name="centre",
    )(middle, one, two)
    early_second = swap(early, "slab", 1)
    early_first = swap(early, "slab", 0)
    late_second = swap(late, "slab", 1)
    late_first = swap(late, "slab", 0)

    right, left, left_early, left_late = pl.pallas_call(
        green_kernel,
        out_shape=[
            jax.ShapeDtypeStruct((3 * wide, wide), BF16),
            jax.ShapeDtypeStruct((width, wide), BF16),
            jax.ShapeDtypeStruct((width, 4 * SPLIT), BF16),
            jax.ShapeDtypeStruct((width, 4 * (width - SPLIT)), BF16),
        ],
        compiler_params=params(),
        cost_estimate=cost(4e9, 12 * block_bytes),
        name="green",
    )(in_hbm(green))

    square = jax.ShapeDtypeStruct((width, wide), F32)
    unit = 2 * width * wide * wide
    partial = pl.pallas_call(
        local_kernel,
        out_shape=square,
        scratch_shapes=[pltpu.VMEM((wide, wide), BF16)],
        compiler_params=params(),
        cost_estimate=cost(4 * unit, 16 * block_bytes),
        name="local",
    )(near_first, early, late, near_second, right, left)

    _, body, rest = packing(reach, width)
    depth = 2 * body + 128
    packed = [pltpu.VMEM((reach, depth), BF16), pltpu.VMEM((depth, wide), BF16)]
    x_first, x_second = pl.pallas_call(
        functools.partial(arrive_kernel, reach),
        in_specs=[smem()] + [pl.BlockSpec(memory_space=pltpu.VMEM)] * 3,
        out_shape=[square, square],
        scratch_shapes=packed if rest else [],
        compiler_params=params(),
        cost_estimate=cost(4 * unit, 16 * block_bytes),
        name="arrive",
    )(roles, from_first, from_second, right)

    partial = pl.pallas_call(
        early_kernel,
        out_shape=square,
        scratch_shapes=[pltpu.VMEM((4 * SPLIT, wide), BF16)],
        compiler_params=params(),
        cost_estimate=cost(3 * unit, 16 * block_bytes),
        name="early",
    )(early_first, early_second, x_first, x_second, right, left_early, partial)

    return pl.pallas_call(
        late_kernel,
        out_specs=hbm(),
        out_shape=pltpu.HBM((1, 1, 2, width, width), F32),
        scratch_shapes=[
            pltpu.VMEM((4 * (width - SPLIT), wide), BF16),
            pltpu.VMEM((2, width, width), F32),
            pltpu.SemaphoreType.DMA((CHUNKS,)),
        ],
        compiler_params=params(),
        cost_estimate=cost(2 * unit, 16 * block_bytes),
        name="late",
    )(late_first, late_second, x_first, x_second, right, left_late, partial)


def solution(mesh):
    in_specs = (
        P("energy", "slab", None, None, None, None),
        P("energy", "slab", None, None, None, None),
        P("energy", "slab", None, None, None),
        P(),
        P(),
        P(),
    )
    out_specs = P("energy", "slab", None, None, None)
    return jax.shard_map(program, mesh=mesh, in_specs=in_specs, out_specs=out_specs, check_vma=False)
```

```python
import functools

import jax
import jax.numpy as jnp
from jax import lax
from jax.experimental import pallas as pl
from jax.experimental.pallas import tpu as pltpu
from jax.sharding import PartitionSpec as P


F32 = jnp.float32
BF16 = jnp.bfloat16
VMEM_LIMIT = 24 * 1024 * 1024
CHUNKS = 3
PIECE = 16
STRIP = 96
LEVELS = (192, 288, 384)
SPLIT = 256


def cost(flops, moved):
    return pl.CostEstimate(flops=int(flops), bytes_accessed=int(moved), transcendentals=0)


def dot(left, right):
    return jnp.dot(left, right, preferred_element_type=F32)


def toward():
    return 1 - 2 * lax.rem(lax.axis_index("slab"), 2)


def matches(slab, offset, off, cnt, rng):
    found = []
    for q in range(off.shape[0]):
        live = (off[q, slab] == offset) & (q < cnt[slab])
        found.append((live.astype(jnp.int32), jnp.where(live, rng[q, slab], 0)))
    return found


def inside(lanes, reach, first):
    return (lanes < jnp.where(first < reach, reach, 0)).astype(F32).astype(BF16)


def strip_sum(sigma, part, reaches, lanes, c):
    slots, _, height, width = sigma.shape
    total = jnp.zeros((height, width), F32)
    for q in range(slots):
        total = total + (sigma[q, part] * inside(lanes, reaches[q], c * height)).astype(F32)
    return total


def packing(reach, width):
    if reach == width:
        return 2 * width, width, 0
    body = reach // 128 * 128
    rest = reach - body
    units = (2 * body // 128 + 1) * (reach // PIECE)
    if folded(rest):
        units -= reach // PIECE // 2
    lanes = 2 * width // 128
    return width + -(-units // lanes) * PIECE, body, rest


def folded(rest):
    return 4 * rest <= 128


def unit_at(group, piece, reach, width):
    lanes = 2 * width // 128
    unit = group * (reach // PIECE) + piece
    row, lane = width + unit // lanes * PIECE, unit % lanes * 128
    return slice(row, row + PIECE), slice(lane, lane + 128)


def widest_small(off, cnt, rng):
    slots = lax.broadcasted_iota(jnp.int32, off.shape, 0)
    live = slots < cnt[...]

    def reach(offset):
        return jnp.max(jnp.where(live & (off[...] == offset), rng[...], 0), axis=0, keepdims=True)

    low = jnp.minimum(reach(-1), reach(-2))
    high = jnp.minimum(reach(1), reach(2))
    return jnp.max(jnp.maximum(low, high))


def near_leads(slab, d, off, cnt, rng):
    near, far = [
        functools.reduce(jnp.maximum, [reach for _, reach in matches(slab, offset, off, cnt, rng)])
        for offset in (d, 2 * d)
    ]
    return near >= far


def side_kernel(off_in, cnt_in, rng_in, sigma, *refs):
    outs, (level, roles) = refs[: 2 * len(LEVELS)], refs[2 * len(LEVELS) : 2 * len(LEVELS) + 2]
    off, cnt, rng, off_v, cnt_v, rng_v, held, sems, table_sems = refs[2 * len(LEVELS) + 2 :]
    slab = lax.axis_index("slab")
    s = toward()
    chunks, slots, _, height, width = held.shape
    moves = (
        (off_in, off_v),
        (cnt_in, cnt_v),
        (rng_in, rng_v),
        (off_in, off),
        (cnt_in, cnt),
        (rng_in, rng),
    )
    tables = [
        pltpu.make_async_copy(src, dst, table_sems.at[n]) for n, (src, dst) in enumerate(moves)
    ]
    copies = [
        pltpu.make_async_copy(
            sigma.at[0, 0, :, :, pl.ds(c * height, height), :], held.at[c], sems.at[c]
        )
        for c in range(chunks)
    ]
    for copy in tables + copies:
        copy.start()
    for copy in tables:
        copy.wait()
    widest = widest_small(off_v, cnt_v, rng_v)
    rank = sum((widest > reach).astype(jnp.int32) for reach in LEVELS[:-1])
    level[0] = rank
    cnt = cnt.at[0]
    last = off.shape[1] - 1
    for n, d in enumerate((s, -s)):
        neighbour = jnp.clip(slab + d, 0, last)
        roles[n] = near_leads(neighbour, -d, off, cnt, rng).astype(jnp.int32)

    merges, messages = [], []
    for d in (s, -s):
        sides = []
        for offset in (d, 2 * d):
            found = matches(slab, offset, off, cnt, rng)
            number = sum(live for live, _ in found)
            which = jnp.int32(0)
            for q in reversed(range(slots)):
                which = jnp.where(found[q][0] > 0, q, which)
            reach = functools.reduce(jnp.maximum, [reach for _, reach in found])
            merges.append((number, which, [reach for _, reach in found]))
            sides.append((which, reach))
        near, far = sides
        leads = near[1] >= far[1]
        big = tuple(jnp.where(leads, u, v) for u, v in zip(near, far))
        small = tuple(jnp.where(leads, v, u) for u, v in zip(near, far))
        messages.append((big, small))

    lanes = lax.broadcasted_iota(jnp.int32, (1, width), 1)
    shared = functools.reduce(jnp.maximum, [number for number, _, _ in merges]) > 1

    @pl.when(shared)
    def _():
        for c in range(chunks):
            copies[c].wait()
            for number, which, reaches in merges:

                @pl.when(number > 1)
                def _():
                    for part in range(2):
                        total = strip_sum(held.at[c], part, reaches, lanes, c)
                        held[c, which, part] = total.astype(BF16)

    for index, reach in enumerate(LEVELS):

        @pl.when(rank == index)
        def _():
            for c in range(chunks):
                pl.when(jnp.logical_not(shared))(copies[c].wait)
                for n, message in enumerate(messages):
                    write_strip(outs[2 * index + n], held.at[c], message, reach, lanes, c)


def write_strip(out, held, message, reach, lanes, c):
    big, small = message
    _, _, height, width = held.shape
    keep_big = inside(lanes, big[1], c * height)
    keep_small = inside(lanes, small[1], c * height)
    whole = [slice(part * width, (part + 1) * width) for part in range(2)]
    for part in range(2):
        out[c * height : (c + 1) * height, whole[part]] = held[big[0], part] * keep_big
    _, body, rest = packing(reach, width)
    if rest == 0:
        for part in range(2):
            first = width + c * height
            out[first : first + height, whole[part]] = held[small[0], part] * keep_small
        return
    if c * height >= reach:
        return
    parts = [
        held[small[0], part, :, : body + 128] * keep_small[:, : body + 128] for part in range(2)
    ]
    tail = parts[0][:, body:].astype(F32) + pltpu.roll(parts[1][:, body:].astype(F32), rest, 1)
    units = [part[:, at : at + 128] for part in parts for at in range(0, body, 128)]
    half = reach // PIECE // 2
    for n in range(height // PIECE):
        piece = c * height // PIECE + n
        rows = slice(n * PIECE, (n + 1) * PIECE)
        for group, unit in enumerate(units):
            out[unit_at(group, piece, reach, width)] = unit[rows]
        if folded(rest) and piece >= half:
            at = unit_at(len(units), piece - half, reach, width)
            out[at] = out[at] + pltpu.roll(tail[rows], 64, 1).astype(BF16)
        else:
            out[unit_at(len(units), piece, reach, width)] = tail[rows].astype(BF16)


def own_kernel(off, cnt, rng, sigma, near_first, near_second, middle):
    slab = lax.axis_index("slab")
    cnt = cnt.at[0]
    _, _, _, width = sigma.shape[2:]
    lanes = lax.broadcasted_iota(jnp.int32, (1, width), 1)
    c = pl.program_id(0)
    for offset, out in ((toward(), near_first), (-toward(), near_second), (0, middle)):
        reaches = [reach for _, reach in matches(slab, offset, off, cnt, rng)]
        for part in range(2):
            total = strip_sum(sigma.at[0, 0], part, reaches, lanes, c)
            out[:, part * width : (part + 1) * width] = total.astype(out.dtype)


def centre_kernel(middle, one, two, early, late):
    width = middle.shape[1] // 2
    for part in range(2):
        mixed = 0.5 * (one[0, 0, part].astype(F32) + two[0, 0, part].astype(F32))
        at = slice(part * width, (part + 1) * width)
        total = (middle[:, at] + mixed.astype(BF16).astype(F32)).astype(BF16)
        early[:, at] = total[:SPLIT]
        late[:, at] = total[SPLIT:]


def green_kernel(green, right, left, left_early, left_late):
    width = green.shape[-1]
    s = toward()
    for slot, o in enumerate((1 + s, 1, 1 - s)):
        real, imag = green[0, 0, o, 0], green[0, 0, o, 1]
        real_t, imag_t = real.T, imag.T
        at = 2 * slot * width
        right[at : at + width, :width] = real_t
        right[at : at + width, width:] = -imag_t
        right[at + width : at + 2 * width, :width] = imag_t
        right[at + width : at + 2 * width, width:] = real_t
        if slot == 1:
            left[:, :width] = real
            left[:, width:] = imag
        else:
            for out, first, last in ((left_early, 0, SPLIT), (left_late, SPLIT, width)):
                height = last - first
                to = slot * height
                out[:, to : to + height] = real[:, first:last]
                out[:, to + height : to + 2 * height] = imag[:, first:last]


def spread(x, out, first):
    height, width = x.shape[0], x.shape[1] // 2
    rounded = x.astype(BF16)
    real, imag = rounded[:, :width], rounded[:, width:]
    out[first : first + height, :width] = real
    out[first : first + height, width:] = imag
    out[first + height : first + 2 * height, :width] = -imag
    out[first + height : first + 2 * height, width:] = real


def local_kernel(near_first, early, late, near_second, right, left, out, held):
    wide = early.shape[1]
    x = dot(near_first[...], right[:wide]) + dot(near_second[...], right[2 * wide :])
    middle = right[wide : 2 * wide]
    x = x + jnp.concatenate([dot(early[...], middle), dot(late[...], middle)], axis=0)
    spread(x, held, 0)
    out[...] = dot(left[...], held[...])


def arrive_kernel(reach, roles, from_first, from_second, right, out_first, out_second, *packed):
    width, wide = out_first.shape
    for n, (message, out, other) in enumerate(
        ((from_first, out_first, 2 * wide), (from_second, out_second, 0))
    ):
        leads = roles[n] > 0
        big_at = pl.multiple_of(jnp.where(leads, wide, other), wide)
        small_at = pl.multiple_of(jnp.where(leads, other, wide), wide)
        total = dot(message[:width], right[pl.ds(big_at, wide)])
        if reach == width:
            out[...] = total + dot(message[width:], right[pl.ds(small_at, wide)])
            continue
        left, down = packed
        _, body, rest = packing(reach, width)
        groups, pieces = 2 * body // 128, reach // PIECE
        for group in range(groups):
            for piece in range(pieces):
                left[piece * PIECE : (piece + 1) * PIECE, group * 128 : (group + 1) * 128] = (
                    message[unit_at(group, piece, reach, width)]
                )
        tails = pieces // 2 if folded(rest) else pieces
        for piece in range(tails):
            left[piece * PIECE : (piece + 1) * PIECE, 2 * body :] = (
                message[unit_at(groups, piece, reach, width)]
            )
        for part in range(2):
            source = pl.multiple_of(small_at + part * width, width)
            down[part * body : (part + 1) * body] = right[pl.ds(source, body)]
            tail = pl.multiple_of(small_at + part * width + body, 128)
            to = 2 * body + part * rest
            down[to : to + rest] = right[pl.ds(tail, rest)]
        if not folded(rest):
            out[:reach] = total[:reach] + dot(left[...], down[: 2 * body + 128])
            out[reach:] = total[reach:]
            continue
        first, last, half = 2 * body, 2 * body + 128, reach // 2
        down[first + 64 : last] = jnp.zeros((64, wide), BF16)
        down[last : last + 64] = jnp.zeros((64, wide), BF16)
        down[last + 64 : last + 128] = down[first : first + 64]
        ends = left[:half, first:last]
        total_small = dot(left[:, :first], down[:first])
        out[:half] = total[:half] + total_small[:half] + dot(ends, down[first:last])
        out[half:reach] = total[half:reach] + total_small[half:] + dot(ends, down[last : last + 128])
        out[reach:] = total[reach:]


def fold(c_first, c_second, x_first, x_second, right, held, first):
    height, wide = c_first.shape
    top = slice(first, first + height)
    spread(x_first[top, :] + dot(c_first[...], right[:wide]), held, 0)
    spread(x_second[top, :] + dot(c_second[...], right[2 * wide :]), held, 2 * height)


def early_kernel(c_first, c_second, x_first, x_second, right, left, partial, out, held):
    fold(c_first, c_second, x_first, x_second, right, held, 0)
    out[...] = partial[...] + dot(left[...], held[...])


def late_kernel(c_first, c_second, x_first, x_second, right, left, partial, out, held, stage, sems):
    width = stage.shape[-1]
    fold(c_first, c_second, x_first, x_second, right, held, SPLIT)
    height = width // CHUNKS
    copies = []
    for c in range(CHUNKS):
        top = pl.ds(c * height, height)
        total = partial[top, :] + dot(left[top, :], held[...])
        stage[0, top, :] = total[:, :width]
        stage[1, top, :] = total[:, width:]
        copies.append(
            pltpu.make_async_copy(stage.at[:, top, :], out.at[0, 0, :, top, :], sems.at[c])
        )
        copies[-1].start()
    for copy in copies:
        copy.wait()


def smem():
    return pl.BlockSpec(memory_space=pltpu.SMEM)


def hbm():
    return pl.BlockSpec(memory_space=pltpu.HBM)


def params():
    return pltpu.CompilerParams(vmem_limit_bytes=VMEM_LIMIT)


def swaps(first, count):
    pairs = []
    for i in range(first, count - 1, 2):
        pairs += [(i, i + 1), (i + 1, i)]
    return pairs


def swap(value, axis, first):
    return lax.ppermute(value, axis, swaps(first, lax.axis_size(axis)))


def in_hbm(value):
    return pltpu.with_memory_space_constraint(value, pltpu.HBM)


def program(green, sigma, phonon, pair_off, pair_count, pair_range):
    width = green.shape[-1]
    wide = 2 * width
    slots = sigma.shape[2]
    tables = (pair_off.T, pair_count[None], pair_range.T)
    block_bytes = 2 * width * wide
    chunks = width // STRIP

    messages = []
    for reach in LEVELS:
        rows = packing(reach, width)[0]
        messages += [jax.ShapeDtypeStruct((rows, wide), BF16)] * 2
    *messages, level, roles = pl.pallas_call(
        side_kernel,
        in_specs=[hbm()] * 4,
        out_specs=[pl.BlockSpec(memory_space=pltpu.VMEM)] * len(messages) + [smem(), smem()],
        out_shape=[
            *messages,
            pltpu.SMEM((1,), jnp.int32),
            pltpu.SMEM((2,), jnp.int32),
        ],
        scratch_shapes=[
            *[pltpu.SMEM(table.shape, jnp.int32) for table in tables],
            *[pltpu.VMEM(table.shape, jnp.int32) for table in tables],
            pltpu.VMEM((chunks, slots, 2, STRIP, width), BF16),
            pltpu.SemaphoreType.DMA((chunks,)),
            pltpu.SemaphoreType.DMA((6,)),
        ],
        compiler_params=params(),
        cost_estimate=cost(3e9, 7 * block_bytes),
        name="side",
    )(*[in_hbm(value) for value in (*tables, sigma)])
    branches = [functools.partial(remainder, reach, 2 * n) for n, reach in enumerate(LEVELS)]
    return lax.switch(level[0], branches, messages, roles, green, sigma, phonon, tables)


def remainder(reach, index, messages, roles, green, sigma, phonon, tables):
    first, second = messages[index : index + 2]
    width = green.shape[-1]
    wide = 2 * width
    slots = sigma.shape[2]
    block_bytes = 2 * width * wide
    from_first = swap(first, "slab", 0)
    from_second = swap(second, "slab", 1)

    one = swap(phonon, "energy", 0)
    two = swap(phonon, "energy", 1)

    tall = pl.BlockSpec((STRIP, wide), lambda c: (c, 0))
    near_first, near_second, middle = pl.pallas_call(
        own_kernel,
        grid=(width // STRIP,),
        in_specs=[
            *[smem()] * 3,
            pl.BlockSpec((1, 1, slots, 2, STRIP, width), lambda c: (0, 0, 0, 0, c, 0)),
        ],
        out_specs=[tall] * 3,
        out_shape=[
            jax.ShapeDtypeStruct((width, wide), BF16),
            jax.ShapeDtypeStruct((width, wide), BF16),
            jax.ShapeDtypeStruct((width, wide), F32),
        ],
        compiler_params=params(),
        cost_estimate=cost(3e9, 7 * block_bytes),
        name="own",
    )(*[in_hbm(value) for value in (*tables, sigma)])

    early, late = pl.pallas_call(
        centre_kernel,
        out_shape=[
            jax.ShapeDtypeStruct((SPLIT, wide), BF16),
            jax.ShapeDtypeStruct((width - SPLIT, wide), BF16),
        ],
        compiler_params=params(),
        cost_estimate=cost(1e9, 5 * block_bytes),
        name="centre",
    )(middle, one, two)
    early_second = swap(early, "slab", 1)
    early_first = swap(early, "slab", 0)
    late_second = swap(late, "slab", 1)
    late_first = swap(late, "slab", 0)

    right, left, left_early, left_late = pl.pallas_call(
        green_kernel,
        out_shape=[
            jax.ShapeDtypeStruct((3 * wide, wide), BF16),
            jax.ShapeDtypeStruct((width, wide), BF16),
            jax.ShapeDtypeStruct((width, 4 * SPLIT), BF16),
            jax.ShapeDtypeStruct((width, 4 * (width - SPLIT)), BF16),
        ],
        compiler_params=params(),
        cost_estimate=cost(4e9, 12 * block_bytes),
        name="green",
    )(in_hbm(green))

    square = jax.ShapeDtypeStruct((width, wide), F32)
    unit = 2 * width * wide * wide
    partial = pl.pallas_call(
        local_kernel,
        out_shape=square,
        scratch_shapes=[pltpu.VMEM((wide, wide), BF16)],
        compiler_params=params(),
        cost_estimate=cost(4 * unit, 16 * block_bytes),
        name="local",
    )(near_first, early, late, near_second, right, left)

    _, body, rest = packing(reach, width)
    depth = 2 * body + 128
    packed = [pltpu.VMEM((reach, depth), BF16), pltpu.VMEM((depth + 128, wide), BF16)]
    x_first, x_second = pl.pallas_call(
        functools.partial(arrive_kernel, reach),
        in_specs=[smem()] + [pl.BlockSpec(memory_space=pltpu.VMEM)] * 3,
        out_shape=[square, square],
        scratch_shapes=packed if rest else [],
        compiler_params=params(),
        cost_estimate=cost(4 * unit, 16 * block_bytes),
        name="arrive",
    )(roles, from_first, from_second, right)

    partial = pl.pallas_call(
        early_kernel,
        out_shape=square,
        scratch_shapes=[pltpu.VMEM((4 * SPLIT, wide), BF16)],
        compiler_params=params(),
        cost_estimate=cost(3 * unit, 16 * block_bytes),
        name="early",
    )(early_first, early_second, x_first, x_second, right, left_early, partial)

    return pl.pallas_call(
        late_kernel,
        out_specs=hbm(),
        out_shape=pltpu.HBM((1, 1, 2, width, width), F32),
        scratch_shapes=[
            pltpu.VMEM((4 * (width - SPLIT), wide), BF16),
            pltpu.VMEM((2, width, width), F32),
            pltpu.SemaphoreType.DMA((CHUNKS,)),
        ],
        compiler_params=params(),
        cost_estimate=cost(2 * unit, 16 * block_bytes),
        name="late",
    )(late_first, late_second, x_first, x_second, right, left_late, partial)


def solution(mesh):
    in_specs = (
        P("energy", "slab", None, None, None, None),
        P("energy", "slab", None, None, None, None),
        P("energy", "slab", None, None, None),
        P(),
        P(),
        P(),
    )
    out_specs = P("energy", "slab", None, None, None)
    return jax.shard_map(program, mesh=mesh, in_specs=in_specs, out_specs=out_specs, check_vma=False)
```

```python
import functools

import jax
import jax.numpy as jnp
from jax import lax
from jax.experimental import pallas as pl
from jax.experimental.pallas import tpu as pltpu
from jax.sharding import PartitionSpec as P


F32 = jnp.float32
BF16 = jnp.bfloat16
VMEM_LIMIT = 24 * 1024 * 1024
CHUNKS = 3
PIECE = 16
STRIP = 96
LEVELS = (192, 288, 384)
SPLIT = 256


def cost(flops, moved):
    return pl.CostEstimate(flops=int(flops), bytes_accessed=int(moved), transcendentals=0)


def dot(left, right):
    return jnp.dot(left, right, preferred_element_type=F32)


def toward():
    return 1 - 2 * lax.rem(lax.axis_index("slab"), 2)


def matches(slab, offset, off, cnt, rng):
    found = []
    for q in range(off.shape[0]):
        live = (off[q, slab] == offset) & (q < cnt[slab])
        found.append((live.astype(jnp.int32), jnp.where(live, rng[q, slab], 0)))
    return found


def inside(lanes, reach, first):
    return (lanes < jnp.where(first < reach, reach, 0)).astype(F32).astype(BF16)


def strip_sum(sigma, part, reaches, lanes, c):
    slots, _, height, width = sigma.shape
    total = jnp.zeros((height, width), F32)
    for q in range(slots):
        total = total + (sigma[q, part] * inside(lanes, reaches[q], c * height)).astype(F32)
    return total


def packing(reach, width):
    if reach == width:
        return 2 * width, width, 0
    body = reach // 128 * 128
    rest = reach - body
    units = (2 * body // 128 + 1) * (reach // PIECE)
    if folded(rest):
        units -= reach // PIECE // 2
    lanes = 2 * width // 128
    return width + -(-units // lanes) * PIECE, body, rest


def folded(rest):
    return 4 * rest <= 128


def unit_at(group, piece, reach, width):
    lanes = 2 * width // 128
    unit = group * (reach // PIECE) + piece
    row, lane = width + unit // lanes * PIECE, unit % lanes * 128
    return slice(row, row + PIECE), slice(lane, lane + 128)


def widest_small(off, cnt, rng):
    slots = lax.broadcasted_iota(jnp.int32, off.shape, 0)
    live = slots < cnt[...]

    def reach(offset):
        return jnp.max(jnp.where(live & (off[...] == offset), rng[...], 0), axis=0, keepdims=True)

    low = jnp.minimum(reach(-1), reach(-2))
    high = jnp.minimum(reach(1), reach(2))
    return jnp.max(jnp.maximum(low, high))


def near_leads(slab, d, off, cnt, rng):
    near, far = [
        functools.reduce(jnp.maximum, [reach for _, reach in matches(slab, offset, off, cnt, rng)])
        for offset in (d, 2 * d)
    ]
    return near >= far


def side_kernel(off_in, cnt_in, rng_in, sigma, *refs):
    outs, (level, roles) = refs[: 2 * len(LEVELS)], refs[2 * len(LEVELS) : 2 * len(LEVELS) + 2]
    off, cnt, rng, off_v, cnt_v, rng_v, held, sems, table_sems = refs[2 * len(LEVELS) + 2 :]
    slab = lax.axis_index("slab")
    s = toward()
    chunks, slots, _, height, width = held.shape
    moves = (
        (off_in, off_v),
        (cnt_in, cnt_v),
        (rng_in, rng_v),
        (off_in, off),
        (cnt_in, cnt),
        (rng_in, rng),
    )
    tables = [
        pltpu.make_async_copy(src, dst, table_sems.at[n]) for n, (src, dst) in enumerate(moves)
    ]

    def pull(c):
        rows = pl.ds(pl.multiple_of(c * height, height), height)
        return pltpu.make_async_copy(sigma.at[0, 0, :, :, rows, :], held.at[c], sems.at[c])

    copies = [pull(c) for c in range(chunks)]
    for copy in tables + copies:
        copy.start()
    for copy in tables:
        copy.wait()
    widest = widest_small(off_v, cnt_v, rng_v)
    rank = sum((widest > reach).astype(jnp.int32) for reach in LEVELS[:-1])
    level[0] = rank
    cnt = cnt.at[0]
    last = off.shape[1] - 1
    for n, d in enumerate((s, -s)):
        neighbour = jnp.clip(slab + d, 0, last)
        roles[n] = near_leads(neighbour, -d, off, cnt, rng).astype(jnp.int32)

    merges, messages = [], []
    for d in (s, -s):
        sides = []
        for offset in (d, 2 * d):
            found = matches(slab, offset, off, cnt, rng)
            number = sum(live for live, _ in found)
            which = jnp.int32(0)
            for q in reversed(range(slots)):
                which = jnp.where(found[q][0] > 0, q, which)
            reach = functools.reduce(jnp.maximum, [reach for _, reach in found])
            merges.append((number, which, [reach for _, reach in found]))
            sides.append((which, reach))
        near, far = sides
        leads = near[1] >= far[1]
        big = tuple(jnp.where(leads, u, v) for u, v in zip(near, far))
        small = tuple(jnp.where(leads, v, u) for u, v in zip(near, far))
        messages.append((big, small))

    lanes = lax.broadcasted_iota(jnp.int32, (1, width), 1)
    shared = functools.reduce(jnp.maximum, [number for number, _, _ in merges]) > 1

    @pl.when(shared)
    def _():
        def merge_strip(c, carry):
            pull(c).wait()
            for number, which, reaches in merges:

                @pl.when(number > 1)
                def _():
                    for part in range(2):
                        total = strip_sum(held.at[c], part, reaches, lanes, c)
                        held[c, which, part] = total.astype(BF16)

            return carry

        lax.fori_loop(0, chunks, merge_strip, 0)

    for index, reach in enumerate(LEVELS):

        @pl.when(rank == index)
        def _():
            for c in range(chunks):
                pl.when(jnp.logical_not(shared))(copies[c].wait)
                for n, message in enumerate(messages):
                    write_strip(outs[2 * index + n], held.at[c], message, reach, lanes, c)


def write_strip(out, held, message, reach, lanes, c):
    big, small = message
    _, _, height, width = held.shape
    keep_big = inside(lanes, big[1], c * height)
    keep_small = inside(lanes, small[1], c * height)
    whole = [slice(part * width, (part + 1) * width) for part in range(2)]
    for part in range(2):
        out[c * height : (c + 1) * height, whole[part]] = held[big[0], part] * keep_big
    _, body, rest = packing(reach, width)
    if rest == 0:
        for part in range(2):
            first = width + c * height
            out[first : first + height, whole[part]] = held[small[0], part] * keep_small
        return
    if c * height >= reach:
        return
    parts = [
        held[small[0], part, :, : body + 128] * keep_small[:, : body + 128] for part in range(2)
    ]
    tail = parts[0][:, body:].astype(F32) + pltpu.roll(parts[1][:, body:].astype(F32), rest, 1)
    units = [part[:, at : at + 128] for part in parts for at in range(0, body, 128)]
    half = reach // PIECE // 2
    for n in range(height // PIECE):
        piece = c * height // PIECE + n
        rows = slice(n * PIECE, (n + 1) * PIECE)
        for group, unit in enumerate(units):
            out[unit_at(group, piece, reach, width)] = unit[rows]
        if folded(rest) and piece >= half:
            at = unit_at(len(units), piece - half, reach, width)
            out[at] = out[at] + pltpu.roll(tail[rows], 64, 1).astype(BF16)
        else:
            out[unit_at(len(units), piece, reach, width)] = tail[rows].astype(BF16)


def own_kernel(off, cnt, rng, sigma, near_first, near_second, middle):
    slab = lax.axis_index("slab")
    cnt = cnt.at[0]
    _, _, _, width = sigma.shape[2:]
    lanes = lax.broadcasted_iota(jnp.int32, (1, width), 1)
    c = pl.program_id(0)
    for offset, out in ((toward(), near_first), (-toward(), near_second), (0, middle)):
        reaches = [reach for _, reach in matches(slab, offset, off, cnt, rng)]
        for part in range(2):
            total = strip_sum(sigma.at[0, 0], part, reaches, lanes, c)
            out[:, part * width : (part + 1) * width] = total.astype(out.dtype)


def centre_kernel(middle, one, two, early, late):
    width = middle.shape[1] // 2
    for part in range(2):
        mixed = 0.5 * (one[0, 0, part].astype(F32) + two[0, 0, part].astype(F32))
        at = slice(part * width, (part + 1) * width)
        total = (middle[:, at] + mixed.astype(BF16).astype(F32)).astype(BF16)
        early[:, at] = total[:SPLIT]
        late[:, at] = total[SPLIT:]


def green_kernel(green, right, left, left_early, left_late):
    width = green.shape[-1]
    s = toward()
    for slot, o in enumerate((1 + s, 1, 1 - s)):
        real, imag = green[0, 0, o, 0], green[0, 0, o, 1]
        real_t, imag_t = real.T, imag.T
        at = 2 * slot * width
        right[at : at + width, :width] = real_t
        right[at : at + width, width:] = -imag_t
        right[at + width : at + 2 * width, :width] = imag_t
        right[at + width : at + 2 * width, width:] = real_t
        if slot == 1:
            left[:, :width] = real
            left[:, width:] = imag
        else:
            for out, first, last in ((left_early, 0, SPLIT), (left_late, SPLIT, width)):
                height = last - first
                to = slot * height
                out[:, to : to + height] = real[:, first:last]
                out[:, to + height : to + 2 * height] = imag[:, first:last]


def spread(x, out, first):
    height, width = x.shape[0], x.shape[1] // 2
    rounded = x.astype(BF16)
    real, imag = rounded[:, :width], rounded[:, width:]
    out[first : first + height, :width] = real
    out[first : first + height, width:] = imag
    out[first + height : first + 2 * height, :width] = -imag
    out[first + height : first + 2 * height, width:] = real


def local_kernel(near_first, early, late, near_second, right, left, out, held):
    wide = early.shape[1]
    x = dot(near_first[...], right[:wide]) + dot(near_second[...], right[2 * wide :])
    middle = right[wide : 2 * wide]
    x = x + jnp.concatenate([dot(early[...], middle), dot(late[...], middle)], axis=0)
    spread(x, held, 0)
    out[...] = dot(left[...], held[...])


def arrive_kernel(reach, roles, from_first, from_second, right, out_first, out_second, *packed):
    width, wide = out_first.shape
    for n, (message, out, other) in enumerate(
        ((from_first, out_first, 2 * wide), (from_second, out_second, 0))
    ):
        leads = roles[n] > 0
        big_at = pl.multiple_of(jnp.where(leads, wide, other), wide)
        small_at = pl.multiple_of(jnp.where(leads, other, wide), wide)
        total = dot(message[:width], right[pl.ds(big_at, wide)])
        if reach == width:
            out[...] = total + dot(message[width:], right[pl.ds(small_at, wide)])
            continue
        left, down = packed
        _, body, rest = packing(reach, width)
        groups, pieces = 2 * body // 128, reach // PIECE
        for group in range(groups):
            for piece in range(pieces):
                left[piece * PIECE : (piece + 1) * PIECE, group * 128 : (group + 1) * 128] = (
                    message[unit_at(group, piece, reach, width)]
                )
        tails = pieces // 2 if folded(rest) else pieces
        for piece in range(tails):
            left[piece * PIECE : (piece + 1) * PIECE, 2 * body :] = (
                message[unit_at(groups, piece, reach, width)]
            )
        for part in range(2):
            source = pl.multiple_of(small_at + part * width, width)
            down[part * body : (part + 1) * body] = right[pl.ds(source, body)]
            tail = pl.multiple_of(small_at + part * width + body, 128)
            to = 2 * body + part * rest
            down[to : to + rest] = right[pl.ds(tail, rest)]
        if not folded(rest):
            out[:reach] = total[:reach] + dot(left[...], down[: 2 * body + 128])
            out[reach:] = total[reach:]
            continue
        first, last, half = 2 * body, 2 * body + 128, reach // 2
        down[first + 64 : last] = jnp.zeros((64, wide), BF16)
        down[last : last + 64] = jnp.zeros((64, wide), BF16)
        down[last + 64 : last + 128] = down[first : first + 64]
        ends = left[:half, first:last]
        total_small = dot(left[:, :first], down[:first])
        out[:half] = total[:half] + total_small[:half] + dot(ends, down[first:last])
        out[half:reach] = total[half:reach] + total_small[half:] + dot(ends, down[last : last + 128])
        out[reach:] = total[reach:]


def fold(c_first, c_second, x_first, x_second, right, held, first):
    height, wide = c_first.shape
    top = slice(first, first + height)
    spread(x_first[top, :] + dot(c_first[...], right[:wide]), held, 0)
    spread(x_second[top, :] + dot(c_second[...], right[2 * wide :]), held, 2 * height)


def early_kernel(c_first, c_second, x_first, x_second, right, left, partial, out, held):
    fold(c_first, c_second, x_first, x_second, right, held, 0)
    out[...] = partial[...] + dot(left[...], held[...])


def late_kernel(c_first, c_second, x_first, x_second, right, left, partial, out, held, stage, sems):
    width = stage.shape[-1]
    fold(c_first, c_second, x_first, x_second, right, held, SPLIT)
    height = width // CHUNKS
    copies = []
    for c in range(CHUNKS):
        top = pl.ds(c * height, height)
        total = partial[top, :] + dot(left[top, :], held[...])
        stage[0, top, :] = total[:, :width]
        stage[1, top, :] = total[:, width:]
        copies.append(
            pltpu.make_async_copy(stage.at[:, top, :], out.at[0, 0, :, top, :], sems.at[c])
        )
        copies[-1].start()
    for copy in copies:
        copy.wait()


def smem():
    return pl.BlockSpec(memory_space=pltpu.SMEM)


def hbm():
    return pl.BlockSpec(memory_space=pltpu.HBM)


def params():
    return pltpu.CompilerParams(vmem_limit_bytes=VMEM_LIMIT)


def swaps(first, count):
    pairs = []
    for i in range(first, count - 1, 2):
        pairs += [(i, i + 1), (i + 1, i)]
    return pairs


def swap(value, axis, first):
    return lax.ppermute(value, axis, swaps(first, lax.axis_size(axis)))


def in_hbm(value):
    return pltpu.with_memory_space_constraint(value, pltpu.HBM)


def program(green, sigma, phonon, pair_off, pair_count, pair_range):
    width = green.shape[-1]
    wide = 2 * width
    slots = sigma.shape[2]
    tables = (pair_off.T, pair_count[None], pair_range.T)
    block_bytes = 2 * width * wide
    chunks = width // STRIP

    messages = []
    for reach in LEVELS:
        rows = packing(reach, width)[0]
        messages += [jax.ShapeDtypeStruct((rows, wide), BF16)] * 2
    *messages, level, roles = pl.pallas_call(
        side_kernel,
        in_specs=[hbm()] * 4,
        out_specs=[pl.BlockSpec(memory_space=pltpu.VMEM)] * len(messages) + [smem(), smem()],
        out_shape=[
            *messages,
            pltpu.SMEM((1,), jnp.int32),
            pltpu.SMEM((2,), jnp.int32),
        ],
        scratch_shapes=[
            *[pltpu.SMEM(table.shape, jnp.int32) for table in tables],
            *[pltpu.VMEM(table.shape, jnp.int32) for table in tables],
            pltpu.VMEM((chunks, slots, 2, STRIP, width), BF16),
            pltpu.SemaphoreType.DMA((chunks,)),
            pltpu.SemaphoreType.DMA((6,)),
        ],
        compiler_params=params(),
        cost_estimate=cost(3e9, 7 * block_bytes),
        name="side",
    )(*[in_hbm(value) for value in (*tables, sigma)])
    branches = [functools.partial(remainder, reach, 2 * n) for n, reach in enumerate(LEVELS)]
    return lax.switch(level[0], branches, messages, roles, green, sigma, phonon, tables)


def remainder(reach, index, messages, roles, green, sigma, phonon, tables):
    first, second = messages[index : index + 2]
    width = green.shape[-1]
    wide = 2 * width
    slots = sigma.shape[2]
    block_bytes = 2 * width * wide
    from_first = swap(first, "slab", 0)
    from_second = swap(second, "slab", 1)

    one = swap(phonon, "energy", 0)
    two = swap(phonon, "energy", 1)

    tall = pl.BlockSpec((STRIP, wide), lambda c: (c, 0))
    near_first, near_second, middle = pl.pallas_call(
        own_kernel,
        grid=(width // STRIP,),
        in_specs=[
            *[smem()] * 3,
            pl.BlockSpec((1, 1, slots, 2, STRIP, width), lambda c: (0, 0, 0, 0, c, 0)),
        ],
        out_specs=[tall] * 3,
        out_shape=[
            jax.ShapeDtypeStruct((width, wide), BF16),
            jax.ShapeDtypeStruct((width, wide), BF16),
            jax.ShapeDtypeStruct((width, wide), F32),
        ],
        compiler_params=params(),
        cost_estimate=cost(3e9, 7 * block_bytes),
        name="own",
    )(*[in_hbm(value) for value in (*tables, sigma)])

    early, late = pl.pallas_call(
        centre_kernel,
        out_shape=[
            jax.ShapeDtypeStruct((SPLIT, wide), BF16),
            jax.ShapeDtypeStruct((width - SPLIT, wide), BF16),
        ],
        compiler_params=params(),
        cost_estimate=cost(1e9, 5 * block_bytes),
        name="centre",
    )(middle, one, two)
    early_second = swap(early, "slab", 1)
    early_first = swap(early, "slab", 0)
    late_second = swap(late, "slab", 1)
    late_first = swap(late, "slab", 0)

    right, left, left_early, left_late = pl.pallas_call(
        green_kernel,
        out_shape=[
            jax.ShapeDtypeStruct((3 * wide, wide), BF16),
            jax.ShapeDtypeStruct((width, wide), BF16),
            jax.ShapeDtypeStruct((width, 4 * SPLIT), BF16),
            jax.ShapeDtypeStruct((width, 4 * (width - SPLIT)), BF16),
        ],
        compiler_params=params(),
        cost_estimate=cost(4e9, 12 * block_bytes),
        name="green",
    )(in_hbm(green))

    square = jax.ShapeDtypeStruct((width, wide), F32)
    unit = 2 * width * wide * wide
    partial = pl.pallas_call(
        local_kernel,
        out_shape=square,
        scratch_shapes=[pltpu.VMEM((wide, wide), BF16)],
        compiler_params=params(),
        cost_estimate=cost(4 * unit, 16 * block_bytes),
        name="local",
    )(near_first, early, late, near_second, right, left)

    _, body, rest = packing(reach, width)
    depth = 2 * body + 128
    packed = [pltpu.VMEM((reach, depth), BF16), pltpu.VMEM((depth + 128, wide), BF16)]
    x_first, x_second = pl.pallas_call(
        functools.partial(arrive_kernel, reach),
        in_specs=[smem()] + [pl.BlockSpec(memory_space=pltpu.VMEM)] * 3,
        out_shape=[square, square],
        scratch_shapes=packed if rest else [],
        compiler_params=params(),
        cost_estimate=cost(4 * unit, 16 * block_bytes),
        name="arrive",
    )(roles, from_first, from_second, right)

    partial = pl.pallas_call(
        early_kernel,
        out_shape=square,
        scratch_shapes=[pltpu.VMEM((4 * SPLIT, wide), BF16)],
        compiler_params=params(),
        cost_estimate=cost(3 * unit, 16 * block_bytes),
        name="early",
    )(early_first, early_second, x_first, x_second, right, left_early, partial)

    return pl.pallas_call(
        late_kernel,
        out_specs=hbm(),
        out_shape=pltpu.HBM((1, 1, 2, width, width), F32),
        scratch_shapes=[
            pltpu.VMEM((4 * (width - SPLIT), wide), BF16),
            pltpu.VMEM((2, width, width), F32),
            pltpu.SemaphoreType.DMA((CHUNKS,)),
        ],
        compiler_params=params(),
        cost_estimate=cost(2 * unit, 16 * block_bytes),
        name="late",
    )(late_first, late_second, x_first, x_second, right, left_late, partial)


def solution(mesh):
    in_specs = (
        P("energy", "slab", None, None, None, None),
        P("energy", "slab", None, None, None, None),
        P("energy", "slab", None, None, None),
        P(),
        P(),
        P(),
    )
    out_specs = P("energy", "slab", None, None, None)
    return jax.shard_map(program, mesh=mesh, in_specs=in_specs, out_specs=out_specs, check_vma=False)
```

```python
import functools

import jax
import jax.numpy as jnp
from jax import lax
from jax.experimental import pallas as pl
from jax.experimental.pallas import tpu as pltpu
from jax.sharding import PartitionSpec as P


F32 = jnp.float32
BF16 = jnp.bfloat16
VMEM_LIMIT = 24 * 1024 * 1024
CHUNKS = 3
PIECE = 16
STRIP = 96
LEVELS = (192, 288, 384)
SPLIT = 256


def cost(flops, moved):
    return pl.CostEstimate(flops=int(flops), bytes_accessed=int(moved), transcendentals=0)


def dot(left, right):
    return jnp.dot(left, right, preferred_element_type=F32)


def toward():
    return 1 - 2 * lax.rem(lax.axis_index("slab"), 2)


def matches(slab, offset, off, cnt, rng):
    found = []
    for q in range(off.shape[0]):
        live = (off[q, slab] == offset) & (q < cnt[slab])
        found.append((live.astype(jnp.int32), jnp.where(live, rng[q, slab], 0)))
    return found


def inside(lanes, reach, first):
    return (lanes < jnp.where(first < reach, reach, 0)).astype(F32).astype(BF16)


def strip_sum(sigma, part, reaches, lanes, c):
    slots, _, height, width = sigma.shape
    total = jnp.zeros((height, width), F32)
    for q in range(slots):
        total = total + (sigma[q, part] * inside(lanes, reaches[q], c * height)).astype(F32)
    return total


def packing(reach, width):
    if reach == width:
        return 2 * width, width, 0
    body = reach // 128 * 128
    rest = reach - body
    units = (2 * body // 128 + 1) * (reach // PIECE)
    if folded(rest):
        units -= reach // PIECE // 2
    lanes = 2 * width // 128
    return width + -(-units // lanes) * PIECE, body, rest


def folded(rest):
    return 4 * rest <= 128


def unit_at(group, piece, reach, width):
    lanes = 2 * width // 128
    unit = group * (reach // PIECE) + piece
    row, lane = width + unit // lanes * PIECE, unit % lanes * 128
    return slice(row, row + PIECE), slice(lane, lane + 128)


def widest_small(off, cnt, rng):
    slots = lax.broadcasted_iota(jnp.int32, off.shape, 0)
    live = slots < cnt[...]

    def reach(offset):
        return jnp.max(jnp.where(live & (off[...] == offset), rng[...], 0), axis=0, keepdims=True)

    low = jnp.minimum(reach(-1), reach(-2))
    high = jnp.minimum(reach(1), reach(2))
    return jnp.max(jnp.maximum(low, high))


def near_leads(slab, d, off, cnt, rng):
    near, far = [
        functools.reduce(jnp.maximum, [reach for _, reach in matches(slab, offset, off, cnt, rng)])
        for offset in (d, 2 * d)
    ]
    return near >= far


def side_kernel(off_in, cnt_in, rng_in, sigma, *refs):
    outs, (level, roles) = refs[: 2 * len(LEVELS)], refs[2 * len(LEVELS) : 2 * len(LEVELS) + 2]
    off, cnt, rng, off_v, cnt_v, rng_v, held, sems, table_sems = refs[2 * len(LEVELS) + 2 :]
    slab = lax.axis_index("slab")
    s = toward()
    chunks, slots, _, height, width = held.shape
    moves = (
        (off_in, off_v),
        (cnt_in, cnt_v),
        (rng_in, rng_v),
        (off_in, off),
        (cnt_in, cnt),
        (rng_in, rng),
    )
    tables = [
        pltpu.make_async_copy(src, dst, table_sems.at[n]) for n, (src, dst) in enumerate(moves)
    ]

    def pull(c):
        rows = pl.ds(pl.multiple_of(c * height, height), height)
        return pltpu.make_async_copy(sigma.at[0, 0, :, :, rows, :], held.at[c], sems.at[c])

    copies = [pull(c) for c in range(chunks)]
    for copy in tables + copies:
        copy.start()
    for copy in tables:
        copy.wait()
    widest = widest_small(off_v, cnt_v, rng_v)
    rank = sum((widest > reach).astype(jnp.int32) for reach in LEVELS[:-1])
    level[0] = rank
    cnt = cnt.at[0]
    last = off.shape[1] - 1
    for n, d in enumerate((s, -s)):
        neighbour = jnp.clip(slab + d, 0, last)
        roles[n] = near_leads(neighbour, -d, off, cnt, rng).astype(jnp.int32)

    merges, messages = [], []
    for d in (s, -s):
        sides = []
        for offset in (d, 2 * d):
            found = matches(slab, offset, off, cnt, rng)
            number = sum(live for live, _ in found)
            which = jnp.int32(0)
            for q in reversed(range(slots)):
                which = jnp.where(found[q][0] > 0, q, which)
            reach = functools.reduce(jnp.maximum, [reach for _, reach in found])
            merges.append((number, which, [reach for _, reach in found]))
            sides.append((which, reach))
        near, far = sides
        leads = near[1] >= far[1]
        big = tuple(jnp.where(leads, u, v) for u, v in zip(near, far))
        small = tuple(jnp.where(leads, v, u) for u, v in zip(near, far))
        messages.append((big, small))

    lanes = lax.broadcasted_iota(jnp.int32, (1, width), 1)
    shared = functools.reduce(jnp.maximum, [number for number, _, _ in merges]) > 1

    @pl.when(shared)
    def _():
        def merge_strip(c, carry):
            pull(c).wait()
            for number, which, reaches in merges:

                @pl.when(number > 1)
                def _():
                    for part in range(2):
                        total = strip_sum(held.at[c], part, reaches, lanes, c)
                        held[c, which, part] = total.astype(BF16)

            return carry

        lax.fori_loop(0, chunks, merge_strip, 0)

    for index, reach in enumerate(LEVELS):

        @pl.when(rank == index)
        def _():
            for c in range(chunks):
                pl.when(jnp.logical_not(shared))(copies[c].wait)
                for n, message in enumerate(messages):
                    write_strip(outs[2 * index + n], held.at[c], message, reach, lanes, c)


def write_strip(out, held, message, reach, lanes, c):
    big, small = message
    _, _, height, width = held.shape
    keep_big = inside(lanes, big[1], c * height)
    keep_small = inside(lanes, small[1], c * height)
    whole = [slice(part * width, (part + 1) * width) for part in range(2)]
    for part in range(2):
        out[c * height : (c + 1) * height, whole[part]] = held[big[0], part] * keep_big
    _, body, rest = packing(reach, width)
    if rest == 0:
        for part in range(2):
            first = width + c * height
            out[first : first + height, whole[part]] = held[small[0], part] * keep_small
        return
    if c * height >= reach:
        return
    parts = [
        held[small[0], part, :, : body + 128] * keep_small[:, : body + 128] for part in range(2)
    ]
    tail = parts[0][:, body:].astype(F32) + pltpu.roll(parts[1][:, body:].astype(F32), rest, 1)
    units = [part[:, at : at + 128] for part in parts for at in range(0, body, 128)]
    half = reach // PIECE // 2
    for n in range(height // PIECE):
        piece = c * height // PIECE + n
        rows = slice(n * PIECE, (n + 1) * PIECE)
        for group, unit in enumerate(units):
            out[unit_at(group, piece, reach, width)] = unit[rows]
        if folded(rest) and piece >= half:
            at = unit_at(len(units), piece - half, reach, width)
            out[at] = out[at] + pltpu.roll(tail[rows], 64, 1).astype(BF16)
        else:
            out[unit_at(len(units), piece, reach, width)] = tail[rows].astype(BF16)


def own_kernel(off, cnt, rng, sigma, near_first, near_second, middle):
    slab = lax.axis_index("slab")
    cnt = cnt.at[0]
    _, _, _, width = sigma.shape[2:]
    lanes = lax.broadcasted_iota(jnp.int32, (1, width), 1)
    c = pl.program_id(0)
    for offset, out in ((toward(), near_first), (-toward(), near_second), (0, middle)):
        reaches = [reach for _, reach in matches(slab, offset, off, cnt, rng)]
        for part in range(2):
            total = strip_sum(sigma.at[0, 0], part, reaches, lanes, c)
            out[:, part * width : (part + 1) * width] = total.astype(out.dtype)


def centre_kernel(middle, one, two, early, late):
    width = middle.shape[1] // 2
    for part in range(2):
        mixed = 0.5 * (one[0, 0, part].astype(F32) + two[0, 0, part].astype(F32))
        at = slice(part * width, (part + 1) * width)
        total = (middle[:, at] + mixed.astype(BF16).astype(F32)).astype(BF16)
        early[:, at] = total[:SPLIT]
        late[:, at] = total[SPLIT:]


def green_kernel(green, right, left, left_early, left_late):
    width = green.shape[-1]
    s = toward()

    def turn(slot, carry):
        o = 1 + s * (1 - slot)
        real_t, imag_t = green[0, 0, o, 0].T, green[0, 0, o, 1].T
        above = pl.ds(pl.multiple_of(2 * slot * width, width), width)
        below = pl.ds(pl.multiple_of((2 * slot + 1) * width, width), width)
        right[above, :width] = real_t
        right[above, width:] = -imag_t
        right[below, :width] = imag_t
        right[below, width:] = real_t
        return carry

    lax.fori_loop(0, 3, turn, 0)
    left[:, :width] = green[0, 0, 1, 0]
    left[:, width:] = green[0, 0, 1, 1]
    for out, first, last in ((left_early, 0, SPLIT), (left_late, SPLIT, width)):
        height = last - first
        for n, o in enumerate((1 + s, 1 - s)):
            for part in range(2):
                to = (2 * n + part) * height
                out[:, to : to + height] = green[0, 0, o, part, :, first:last]


def spread(x, out, first):
    height, width = x.shape[0], x.shape[1] // 2
    rounded = x.astype(BF16)
    real, imag = rounded[:, :width], rounded[:, width:]
    out[first : first + height, :width] = real
    out[first : first + height, width:] = imag
    out[first + height : first + 2 * height, :width] = -imag
    out[first + height : first + 2 * height, width:] = real


def local_kernel(near_first, early, late, near_second, right, left, out, held):
    wide = early.shape[1]
    x = dot(near_first[...], right[:wide]) + dot(near_second[...], right[2 * wide :])
    middle = right[wide : 2 * wide]
    x = x + jnp.concatenate([dot(early[...], middle), dot(late[...], middle)], axis=0)
    spread(x, held, 0)
    out[...] = dot(left[...], held[...])


def arrive_kernel(reach, roles, from_first, from_second, right, out_first, out_second, *packed):
    width, wide = out_first.shape
    for n, (message, out, other) in enumerate(
        ((from_first, out_first, 2 * wide), (from_second, out_second, 0))
    ):
        leads = roles[n] > 0
        big_at = pl.multiple_of(jnp.where(leads, wide, other), wide)
        small_at = pl.multiple_of(jnp.where(leads, other, wide), wide)
        total = dot(message[:width], right[pl.ds(big_at, wide)])
        if reach == width:
            out[...] = total + dot(message[width:], right[pl.ds(small_at, wide)])
            continue
        left, down = packed
        _, body, rest = packing(reach, width)
        groups, pieces = 2 * body // 128, reach // PIECE
        for group in range(groups):
            for piece in range(pieces):
                left[piece * PIECE : (piece + 1) * PIECE, group * 128 : (group + 1) * 128] = (
                    message[unit_at(group, piece, reach, width)]
                )
        tails = pieces // 2 if folded(rest) else pieces
        for piece in range(tails):
            left[piece * PIECE : (piece + 1) * PIECE, 2 * body :] = (
                message[unit_at(groups, piece, reach, width)]
            )
        for part in range(2):
            source = pl.multiple_of(small_at + part * width, width)
            down[part * body : (part + 1) * body] = right[pl.ds(source, body)]
            tail = pl.multiple_of(small_at + part * width + body, 128)
            to = 2 * body + part * rest
            down[to : to + rest] = right[pl.ds(tail, rest)]
        if not folded(rest):
            out[:reach] = total[:reach] + dot(left[...], down[: 2 * body + 128])
            out[reach:] = total[reach:]
            continue
        first, last, half = 2 * body, 2 * body + 128, reach // 2
        down[first + 64 : last] = jnp.zeros((64, wide), BF16)
        down[last : last + 64] = jnp.zeros((64, wide), BF16)
        down[last + 64 : last + 128] = down[first : first + 64]
        ends = left[:half, first:last]
        total_small = dot(left[:, :first], down[:first])
        out[:half] = total[:half] + total_small[:half] + dot(ends, down[first:last])
        out[half:reach] = total[half:reach] + total_small[half:] + dot(ends, down[last : last + 128])
        out[reach:] = total[reach:]


def fold(c_first, c_second, x_first, x_second, right, held, first):
    height, wide = c_first.shape
    top = slice(first, first + height)
    spread(x_first[top, :] + dot(c_first[...], right[:wide]), held, 0)
    spread(x_second[top, :] + dot(c_second[...], right[2 * wide :]), held, 2 * height)


def early_kernel(c_first, c_second, x_first, x_second, right, left, partial, out, held):
    fold(c_first, c_second, x_first, x_second, right, held, 0)
    out[...] = partial[...] + dot(left[...], held[...])


def late_kernel(c_first, c_second, x_first, x_second, right, left, partial, out, held, stage, sems):
    width = stage.shape[-1]
    fold(c_first, c_second, x_first, x_second, right, held, SPLIT)
    height = width // CHUNKS
    copies = []
    for c in range(CHUNKS):
        top = pl.ds(c * height, height)
        total = partial[top, :] + dot(left[top, :], held[...])
        stage[0, top, :] = total[:, :width]
        stage[1, top, :] = total[:, width:]
        copies.append(
            pltpu.make_async_copy(stage.at[:, top, :], out.at[0, 0, :, top, :], sems.at[c])
        )
        copies[-1].start()
    for copy in copies:
        copy.wait()


def smem():
    return pl.BlockSpec(memory_space=pltpu.SMEM)


def hbm():
    return pl.BlockSpec(memory_space=pltpu.HBM)


def params():
    return pltpu.CompilerParams(vmem_limit_bytes=VMEM_LIMIT)


def swaps(first, count):
    pairs = []
    for i in range(first, count - 1, 2):
        pairs += [(i, i + 1), (i + 1, i)]
    return pairs


def swap(value, axis, first):
    return lax.ppermute(value, axis, swaps(first, lax.axis_size(axis)))


def in_hbm(value):
    return pltpu.with_memory_space_constraint(value, pltpu.HBM)


def program(green, sigma, phonon, pair_off, pair_count, pair_range):
    width = green.shape[-1]
    wide = 2 * width
    slots = sigma.shape[2]
    tables = (pair_off.T, pair_count[None], pair_range.T)
    block_bytes = 2 * width * wide
    chunks = width // STRIP

    messages = []
    for reach in LEVELS:
        rows = packing(reach, width)[0]
        messages += [jax.ShapeDtypeStruct((rows, wide), BF16)] * 2
    *messages, level, roles = pl.pallas_call(
        side_kernel,
        in_specs=[hbm()] * 4,
        out_specs=[pl.BlockSpec(memory_space=pltpu.VMEM)] * len(messages) + [smem(), smem()],
        out_shape=[
            *messages,
            pltpu.SMEM((1,), jnp.int32),
            pltpu.SMEM((2,), jnp.int32),
        ],
        scratch_shapes=[
            *[pltpu.SMEM(table.shape, jnp.int32) for table in tables],
            *[pltpu.VMEM(table.shape, jnp.int32) for table in tables],
            pltpu.VMEM((chunks, slots, 2, STRIP, width), BF16),
            pltpu.SemaphoreType.DMA((chunks,)),
            pltpu.SemaphoreType.DMA((6,)),
        ],
        compiler_params=params(),
        cost_estimate=cost(3e9, 7 * block_bytes),
        name="side",
    )(*[in_hbm(value) for value in (*tables, sigma)])
    branches = [functools.partial(remainder, reach, 2 * n) for n, reach in enumerate(LEVELS)]
    return lax.switch(level[0], branches, messages, roles, green, sigma, phonon, tables)


def remainder(reach, index, messages, roles, green, sigma, phonon, tables):
    first, second = messages[index : index + 2]
    width = green.shape[-1]
    wide = 2 * width
    slots = sigma.shape[2]
    block_bytes = 2 * width * wide
    from_first = swap(first, "slab", 0)
    from_second = swap(second, "slab", 1)

    one = swap(phonon, "energy", 0)
    two = swap(phonon, "energy", 1)

    tall = pl.BlockSpec((STRIP, wide), lambda c: (c, 0))
    near_first, near_second, middle = pl.pallas_call(
        own_kernel,
        grid=(width // STRIP,),
        in_specs=[
            *[smem()] * 3,
            pl.BlockSpec((1, 1, slots, 2, STRIP, width), lambda c: (0, 0, 0, 0, c, 0)),
        ],
        out_specs=[tall] * 3,
        out_shape=[
            jax.ShapeDtypeStruct((width, wide), BF16),
            jax.ShapeDtypeStruct((width, wide), BF16),
            jax.ShapeDtypeStruct((width, wide), F32),
        ],
        compiler_params=params(),
        cost_estimate=cost(3e9, 7 * block_bytes),
        name="own",
    )(*[in_hbm(value) for value in (*tables, sigma)])

    early, late = pl.pallas_call(
        centre_kernel,
        out_shape=[
            jax.ShapeDtypeStruct((SPLIT, wide), BF16),
            jax.ShapeDtypeStruct((width - SPLIT, wide), BF16),
        ],
        compiler_params=params(),
        cost_estimate=cost(1e9, 5 * block_bytes),
        name="centre",
    )(middle, one, two)
    early_second = swap(early, "slab", 1)
    early_first = swap(early, "slab", 0)
    late_second = swap(late, "slab", 1)
    late_first = swap(late, "slab", 0)

    right, left, left_early, left_late = pl.pallas_call(
        green_kernel,
        out_shape=[
            jax.ShapeDtypeStruct((3 * wide, wide), BF16),
            jax.ShapeDtypeStruct((width, wide), BF16),
            jax.ShapeDtypeStruct((width, 4 * SPLIT), BF16),
            jax.ShapeDtypeStruct((width, 4 * (width - SPLIT)), BF16),
        ],
        compiler_params=params(),
        cost_estimate=cost(4e9, 12 * block_bytes),
        name="green",
    )(in_hbm(green))

    square = jax.ShapeDtypeStruct((width, wide), F32)
    unit = 2 * width * wide * wide
    partial = pl.pallas_call(
        local_kernel,
        out_shape=square,
        scratch_shapes=[pltpu.VMEM((wide, wide), BF16)],
        compiler_params=params(),
        cost_estimate=cost(4 * unit, 16 * block_bytes),
        name="local",
    )(near_first, early, late, near_second, right, left)

    _, body, rest = packing(reach, width)
    depth = 2 * body + 128
    packed = [pltpu.VMEM((reach, depth), BF16), pltpu.VMEM((depth + 128, wide), BF16)]
    x_first, x_second = pl.pallas_call(
        functools.partial(arrive_kernel, reach),
        in_specs=[smem()] + [pl.BlockSpec(memory_space=pltpu.VMEM)] * 3,
        out_shape=[square, square],
        scratch_shapes=packed if rest else [],
        compiler_params=params(),
        cost_estimate=cost(4 * unit, 16 * block_bytes),
        name="arrive",
    )(roles, from_first, from_second, right)

    partial = pl.pallas_call(
        early_kernel,
        out_shape=square,
        scratch_shapes=[pltpu.VMEM((4 * SPLIT, wide), BF16)],
        compiler_params=params(),
        cost_estimate=cost(3 * unit, 16 * block_bytes),
        name="early",
    )(early_first, early_second, x_first, x_second, right, left_early, partial)

    return pl.pallas_call(
        late_kernel,
        out_specs=hbm(),
        out_shape=pltpu.HBM((1, 1, 2, width, width), F32),
        scratch_shapes=[
            pltpu.VMEM((4 * (width - SPLIT), wide), BF16),
            pltpu.VMEM((2, width, width), F32),
            pltpu.SemaphoreType.DMA((CHUNKS,)),
        ],
        compiler_params=params(),
        cost_estimate=cost(2 * unit, 16 * block_bytes),
        name="late",
    )(late_first, late_second, x_first, x_second, right, left_late, partial)


def solution(mesh):
    in_specs = (
        P("energy", "slab", None, None, None, None),
        P("energy", "slab", None, None, None, None),
        P("energy", "slab", None, None, None),
        P(),
        P(),
        P(),
    )
    out_specs = P("energy", "slab", None, None, None)
    return jax.shard_map(program, mesh=mesh, in_specs=in_specs, out_specs=out_specs, check_vma=False)
```
